32 devices in a mesh: groups: 2 (over y), seq: 4 (over z), head: 2 (over x), rep: 2 (over core).
Axes of the slice: x: 2, y: 2, z: 4, core: 2. Of those that a mesh axis runs over, the one named last changes fastest.
Arguments:
- queries: bfloat16 [2048, 6144], P(('groups', 'seq', 'rep'), 'head'), parts along dimension 0, may hold values from -150 to 150
- key_tokens: bfloat16 [2048, 6144], P(('groups', 'seq', 'rep'), 'head'), parts along dimension 0, may hold values from -6 to 6
- value_tokens: bfloat16 [2048, 6144], P(('groups', 'seq', 'rep'), 'head'), parts along dimension 0, may hold values from -6 to 6
- stream: bfloat16 [2048, 6144], P(('groups', 'seq', 'rep'), 'head'), parts along dimension 0, may hold values from -6 to 6
- norm_gain: float32 [6144], P('head'), may hold values from 0.1 to 1.9
- latent_weight: bfloat16 [6144, 64], P('head'), may hold values from -0.078125 to 0.078125
- tile_pool: bfloat16 [8, 64, 2, 128], P(('groups', 'seq')), parts along dimension 0, may hold values from -6 to 6
- tile_position: int32 [8], P('groups'), parts along dimension 0, may hold values from 0 to 3, each once
- lift_weight: bfloat16 [64, 512], P(None, ('head', 'rep')), may hold values from -0.75 to 0.75
- lift_bias: float32 [512], P(('head', 'rep')), may hold values from -3 to 3
- conv_weight: bfloat16 [2, 27, 512, 512], P(None, None, ('head', 'rep')), may hold values from -0.0546875 to 0.0546875
Outputs:
- hidden: bfloat16 [2048, 6144], P(('groups', 'seq', 'rep'), 'head'), parts along dimension 0
- latents: float32 [2048, 64], P(('groups', 'seq', 'rep')), parts along dimension 0
- decoded: float32 [1024, 2, 4, 128], P(('groups', 'head', 'rep'), None, 'seq'), parts along dimension 0
The draws below stay inside these ranges and needn't reach their ends.
There are 2 independent parts, one for each index of `groups`. The reference program is written for one: setup_inputs(seed, part) draws one part's arguments, and reference() takes and returns one part's arrays. A program takes and returns all parts, laid end to end along the dimension named above; an argument that names none is the same for every part. Nothing has to cross between parts.
Inputs may be any that keep to these rules, and one draw needn't show every extreme that they name: `tile_position`: each of the 4 grid rows is named by exactly one pool tile.
All inputs are finite; a program needn't handle non-finite values.
Results may differ from the reference program's by a relative error of at most 0.01.
Values may be sent and summed in bfloat16 or wider, within the bound.
A program may use at most 128 MiB of HBM per device.

```python
import math
import jax
import jax.numpy as jnp
from jax import lax

HEADS = 48
HEAD_DIM = 128
WIDTH = 6144
LATENT = 64
CHANNELS = 512
FRAMES = 2
COLS = 128
DLAYERS = 2
TOKENS = 1024
TILES = 4


def key_draw(key):
    return jnp.clip(jax.random.normal(jax.random.fold_in(key, 102), (TOKENS, WIDTH), jnp.float32), -6.0, 6.0)


def draw_key_tokens(key, part):
    drawn = key_draw(key)
    return drawn.astype(jnp.bfloat16)


def draw_queries(key, part):
    drawn = jnp.clip(2.5 * jax.random.normal(jax.random.fold_in(key, 104), (TOKENS, WIDTH), jnp.float32), -15.0, 15.0)
    return drawn.astype(jnp.bfloat16)


def block_scale(stream_key, extent, pieces, smallest, largest):
    loudness = 1.0
    for axis_at, shards_of in pieces:
        steps = jax.random.uniform(jax.random.fold_in(jax.random.fold_in(stream_key, 6), axis_at), (shards_of,), jnp.float32, smallest / len(pieces), largest / len(pieces))
        loudness = loudness * jnp.repeat(jnp.exp(steps), extent[axis_at] // shards_of).reshape((-1,) + (1,) * (len(extent) - 1 - axis_at))
    return loudness


def noise(own_key, extent, spread, limit, cuts=(), kind=jnp.bfloat16):
    entries = spread * jax.random.normal(own_key, extent, jnp.float32)
    if cuts:
        entries = entries * block_scale(own_key, extent, cuts, -0.22, 0.18)
    return jnp.clip(entries, -limit, limit).astype(kind)


def setup_inputs(seed: int = 0, part: int = 0) -> dict:
    key_of = jax.random.split(jax.random.key(seed), 12)
    own_keys = jax.random.split(jax.random.fold_in(key_of[11], part), 12)
    queries = draw_queries(jax.random.fold_in(jax.random.fold_in(key_of[11], part), 71), part)
    key_tokens = draw_key_tokens(jax.random.fold_in(jax.random.fold_in(key_of[11], part), 71), part)
    value_tokens = noise(own_keys[2], (TOKENS, WIDTH), 1.0, 6.0, ((0, 8), (1, 2)))
    stream = noise(own_keys[3], (TOKENS, WIDTH), 1.0, 6.0, ((0, 8), (1, 2)))
    norm_gain = jnp.clip(1.0 + 0.18 * jax.random.normal(key_of[4], (WIDTH,), jnp.float32), 0.1, 1.9)
    latent_weight = noise(key_of[5], (WIDTH, LATENT), WIDTH ** -0.5, 0.078125, ((0, 2),))
    tile_pool = noise(own_keys[6], (TILES, LATENT, FRAMES, COLS), 1.0, 6.0, ((0, 4),))
    tile_position = jax.random.permutation(own_keys[7], TILES).astype(jnp.int32)
    lift_weight = noise(key_of[8], (LATENT, CHANNELS), LATENT ** -0.5, 0.75, ((1, 4),))
    lift_bias = noise(key_of[9], (CHANNELS,), 0.5, 3.0, ((0, 4),), jnp.float32)
    conv_weight = noise(key_of[10], (DLAYERS, 27, CHANNELS, CHANNELS), (27 * CHANNELS) ** -0.5, 0.0546875, ((2, 4),))
    return {"queries": queries, "key_tokens": key_tokens, "value_tokens": value_tokens, "stream": stream, "norm_gain": norm_gain, "latent_weight": latent_weight, "tile_pool": tile_pool, "tile_position": tile_position, "lift_weight": lift_weight, "lift_bias": lift_bias, "conv_weight": conv_weight}


epsilon = 1e-06

def head_attention(operands):
    query_head, key_head, value_head = operands
    scores = jnp.dot(query_head, key_head.T, preferred_element_type=jnp.float32) * (1.0 / math.sqrt(HEAD_DIM))
    row_peak = lax.optimization_barrier(jnp.max(scores, axis=1, keepdims=True))
    exponent = jnp.exp(scores - row_peak)
    weights = exponent.astype(jnp.bfloat16)
    summed = jnp.dot(weights, value_head, preferred_element_type=jnp.float32)
    return (summed / lax.optimization_barrier(jnp.sum(exponent, axis=1, keepdims=True))).astype(jnp.bfloat16)

def by_heads(matrix):
    return jnp.transpose(matrix.reshape(TOKENS, HEADS, HEAD_DIM), (1, 0, 2))

def reference(queries, key_tokens, value_tokens, stream, norm_gain, latent_weight, tile_pool, tile_position, lift_weight, lift_bias, conv_weight):
    attended = lax.map(head_attention, (by_heads(queries), by_heads(key_tokens), by_heads(value_tokens)))
    attended = jnp.transpose(attended, (1, 0, 2)).reshape(TOKENS, WIDTH)
    hidden = (stream.astype(jnp.float32) + attended.astype(jnp.float32)).astype(jnp.bfloat16)
    widened = hidden.astype(jnp.float32)
    scaled = (widened * norm_gain).astype(jnp.bfloat16)
    projected = jnp.dot(scaled, latent_weight, preferred_element_type=jnp.float32)
    squares = lax.optimization_barrier(jnp.sum(widened * widened, axis=1))
    latents = projected * lax.rsqrt(squares / WIDTH + epsilon)[:, None]
    latent_grid = jnp.zeros((LATENT, FRAMES, TILES, COLS), jnp.bfloat16)
    latent_grid = latent_grid.at[:, :, tile_position.astype(jnp.int32), :].set(jnp.transpose(tile_pool, (1, 2, 0, 3)))
    feature_map = jnp.dot(lift_weight.T, latent_grid.reshape(LATENT, -1), preferred_element_type=jnp.float32) + lift_bias[:, None]
    for layer_index in range(DLAYERS):
        active = jax.nn.silu(feature_map).astype(jnp.bfloat16).reshape(CHANNELS, FRAMES, TILES, COLS)
        padded = jnp.pad(active, ((0, 0), (1, 1), (1, 1), (1, 1)))
        update = jnp.zeros((CHANNELS, FRAMES * TILES * COLS), jnp.float32)
        for frame_off in range(3):
            for row_off in range(3):
                for col_off in range(3):
                    window = padded[:, frame_off:frame_off + FRAMES, row_off:row_off + TILES, col_off:col_off + COLS].reshape(CHANNELS, -1)
                    tap_weight = conv_weight[layer_index, frame_off * 9 + row_off * 3 + col_off]
                    update = update + lax.dot_general(tap_weight, window, (((1,), (0,)), ((), ())), preferred_element_type=jnp.float32)
        feature_map = feature_map + update
    decoded = feature_map.reshape(CHANNELS, FRAMES, TILES, COLS)
    return (hidden, latents, decoded)
```

```python
import functools
import math

import jax
import jax.numpy as jnp
from jax import lax
from jax.experimental import pallas as pl
from jax.experimental.pallas import tpu as pltpu
from jax.sharding import PartitionSpec as P

HEAD_DIM = 128
WIDTH = 6144


epsilon = 1e-06
negative = -1e30


def padded(shard, sides, width):
    for axis, dim in sides:
        peers, length = (lax.axis_size(axis), shard.shape[dim])
        up = [(i, (i + 1) % peers) for i in range(peers - 1)]
        down = [(j, i) for i, j in up]
        last = lax.slice_in_dim(shard, length - width, length, axis=dim)
        leading = lax.slice_in_dim(shard, 0, width, axis=dim)
        before = lax.ppermute(last, axis, up)
        after = lax.ppermute(leading, axis, down)
        shard = jnp.concatenate([before, shard, after], axis=dim)
    return shard


def prepare(block_rows):
    row_count = block_rows.shape[0]
    head_count = block_rows.shape[1] // HEAD_DIM
    query_heads = block_rows.reshape(row_count, head_count, HEAD_DIM)
    initial = (
        jnp.full((head_count, row_count), negative, jnp.float32),
        jnp.zeros((head_count, row_count), jnp.float32),
        jnp.zeros((head_count, row_count, HEAD_DIM), jnp.float32),
    )
    return (query_heads, initial)


def make_update(query_heads, state, pieces):
    head_count = query_heads.shape[1]
    factor = 1.0 / math.sqrt(HEAD_DIM)
    running_max, running_sum, accum = state
    key_piece, value_piece = pieces
    piece_rows = key_piece.shape[0]
    key_heads = key_piece.reshape(piece_rows, head_count, HEAD_DIM)
    value_heads = value_piece.reshape(piece_rows, head_count, HEAD_DIM)
    scores = (
        jnp.einsum("qhd,khd->hqk", query_heads, key_heads, preferred_element_type=jnp.float32)
        * factor
    )
    new_max = jnp.maximum(running_max, jnp.max(scores, axis=2))
    exponent = jnp.exp(scores - new_max[:, :, None])
    running_sum = jnp.sum(exponent, axis=2)
    accum = jnp.einsum(
        "hqk,khd->hqd",
        exponent.astype(jnp.bfloat16),
        value_heads,
        preferred_element_type=jnp.float32,
    )
    return (new_max, running_sum, accum)


def finish(state):
    running_max, running_sum, accum = state
    result = accum / running_sum[:, :, None]
    return jnp.transpose(result, (1, 0, 2)).reshape(result.shape[1], -1).astype(jnp.bfloat16)


def shift_columns(window, col_shift):
    if col_shift == 0:
        return window
    edge = jnp.zeros(window.shape[:-1] + (1,), window.dtype)
    if col_shift < 0:
        return jnp.concatenate([edge, window[..., :-1]], axis=-1)
    return jnp.concatenate([window[..., 1:], edge], axis=-1)


def tap_sum(running, piece_block, layer_weight):
    piece_rows = piece_block.shape[0]
    frames = piece_block.shape[1]
    band_rows = piece_block.shape[2] - 2
    framed = jnp.pad(piece_block, ((0, 0), (1, 1), (0, 0), (0, 0)))
    for frame_off in range(3):
        for row_off in range(3):
            for col_off in range(3):
                window = shift_columns(
                    framed[:, frame_off : frame_off + frames, row_off : row_off + band_rows, :],
                    col_off - 1,
                )
                tap_weight = layer_weight[frame_off * 9 + row_off * 3 + col_off]
                running = running + lax.dot_general(
                    tap_weight,
                    window.reshape(piece_rows, -1),
                    (((1,), (0,)), ((), ())),
                    preferred_element_type=jnp.float32,
                )
    return running


def make_pick(tile_position, own_rows, piece_block):
    selector = (own_rows[:, None] == tile_position[None, :]).astype(jnp.bfloat16)
    return jnp.einsum("tp,plfc->lftc", selector, piece_block, preferred_element_type=jnp.float32)


MESH = pl.DeviceIdType.MESH


def fused_kernel(
    seq_size, rep_size, head_size, full_width,
    q_hbm, k_hbm, v_hbm, stream_hbm, gain_hbm, lw_hbm,
    tile_hbm, place_hbm, lift_hbm, bias_hbm, conv_hbm,
    hid_ref, lat_ref, dec_ref,
    q_ref, k_ref, v_ref, stream_ref, gain_ref, lw_ref, place_ref,
    qkv, obuf, att, part, part_in,
    tiles, lifts, biases, taps, act1, act2, feat, acc,
    ready, ready_mate,
    send_sem, recv_sem, osend_sem, orecv_sem, psend_sem, precv_sem,
    load_sem, side_sem, tap_sem, dsend_sem, drecv_sem,
):
    seq, rep, head = (lax.axis_index(a) for a in ("seq", "rep", "head"))
    count = seq_size * rep_size
    me = seq * rep_size + rep
    rows = q_ref.shape[0]
    own_heads = qkv.shape[0]
    others = count - 1
    factor = 1.0 / math.sqrt(HEAD_DIM)
    quarter = head * rep_size + rep
    sources = (q_ref, k_ref, v_ref)

    stretch = count * HEAD_DIM
    loads = []
    for h in range(own_heads):
        cols = pl.ds(h * stretch, stretch)
        loads.append([
            pltpu.make_async_copy(origin.at[:, cols], source.at[:, cols], load_sem.at[3 * h + i])
            for i, (origin, source) in enumerate(zip((q_hbm, k_hbm, v_hbm), sources))
        ])
    for load in loads[0]:
        load.start()

    barrier = pltpu.get_barrier_semaphore()
    for e in range(1, rep_size):
        pl.semaphore_signal(
            barrier, inc=1, device_id={"rep": lax.rem(rep + e, rep_size)}, device_id_type=MESH
        )
    for k in range(1, seq_size):
        @pl.when(seq + k < seq_size)
        def _():
            for r in range(rep_size):
                pl.semaphore_signal(
                    barrier, inc=1, device_id={"seq": seq + k, "rep": r}, device_id_type=MESH
                )
    for k in range(1, head_size):
        @pl.when(head + k < head_size)
        def _():
            for r in range(rep_size):
                pl.semaphore_signal(
                    barrier, inc=1, device_id={"head": head + k, "rep": r}, device_id_type=MESH
                )
    pl.semaphore_wait(barrier, rep_size - 1 + rep_size * (seq + head))
    for k in range(1, seq_size):
        @pl.when(seq >= k)
        def _():
            for r in range(rep_size):
                pl.semaphore_signal(
                    ready.at[k - 1], inc=1, device_id={"seq": seq - k, "rep": r},
                    device_id_type=MESH,
                )
    for k in range(1, head_size):
        @pl.when(head >= k)
        def _():
            for r in range(rep_size):
                pl.semaphore_signal(
                    ready_mate.at[k - 1], inc=1, device_id={"head": head - k, "rep": r},
                    device_id_type=MESH,
                )

    share = tiles.shape[1] // (head_size * rep_size)
    my_share = pl.ds(pl.multiple_of(quarter * share, share), share)
    sides = [
        pltpu.make_async_copy(origin, target, side_sem.at[i])
        for i, (origin, target) in enumerate((
            (tile_hbm.at[0, my_share], tiles.at[seq, my_share]),
            (lift_hbm, lifts.at[quarter]),
            (bias_hbm, biases.at[quarter]),
            (place_hbm, place_ref),
            (stream_hbm, stream_ref),
            (gain_hbm, gain_ref),
            (lw_hbm, lw_ref),
        ))
    ]
    for side in sides[:4]:
        side.start()

    def arrived(ref, sem):
        pltpu.make_async_copy(ref, ref, sem).wait()

    def send(source, target, index, device):
        pltpu.make_async_remote_copy(
            src_ref=source, dst_ref=target,
            send_sem=dsend_sem.at[index], recv_sem=drecv_sem.at[index],
            device_id=device, device_id_type=MESH,
        ).start()

    my_rows = pl.ds(pl.multiple_of(me * rows, rows), rows)

    def block_of(h, place):
        return pl.ds(pl.multiple_of((h * count + place) * HEAD_DIM, HEAD_DIM), HEAD_DIM)

    def send_one(h, target, r):
        columns = block_of(h, target * rep_size + r)
        for i, source in enumerate(sources):
            pltpu.make_async_remote_copy(
                src_ref=source.at[:, columns],
                dst_ref=qkv.at[h, i, my_rows, :],
                send_sem=send_sem,
                recv_sem=recv_sem.at[h],
                device_id={"seq": target, "rep": r},
                device_id_type=MESH,
            ).start()

    def send_head(h):
        for k in (2, 1, 3):
            @pl.when(seq >= k)
            def _():
                if h == 0:
                    send(tiles.at[seq, my_share], tiles.at[seq, my_share], 0, {"seq": seq - k})
                for r in range(rep_size):
                    send_one(h, seq - k, r)
        for k in range(1, seq_size):
            @pl.when(seq + k < seq_size)
            def _():
                if h == 0:
                    pl.semaphore_wait(ready.at[k - 1], rep_size)
                    send(tiles.at[seq, my_share], tiles.at[seq, my_share], 0, {"seq": seq + k})
                for r in range(rep_size):
                    send_one(h, seq + k, r)
        for e in range(1, rep_size):
            send_one(h, seq, lax.rem(rep + e, rep_size))

    for load in loads[0]:
        load.wait()
    sides[0].wait()
    send_head(0)
    for pending in loads[1:]:
        for load in pending:
            load.start()
    tap_copy = pltpu.make_async_copy(conv_hbm, taps, tap_sem)
    tap_copy.start()
    for side in sides[4:]:
        side.start()
    for h in range(1, own_heads):
        for load in loads[h]:
            load.wait()
        send_head(h)

    mates = [
        {"head": lax.rem(head + d, head_size), "rep": lax.rem(rep + e, rep_size)}
        for d in range(head_size) for e in range(rep_size) if (d, e) != (0, 0)
    ]
    for k in range(1, head_size):
        @pl.when(head + k < head_size)
        def _():
            pl.semaphore_wait(ready_mate.at[k - 1], rep_size)
    sides[1].wait()
    sides[2].wait()
    for mate in mates:
        send(lifts.at[quarter], lifts.at[quarter], 1, mate)
        send(biases.at[quarter], biases.at[quarter], 2, mate)
    pieces = len(mates)
    arrived(tiles.at[pl.ds(0, seq_size - 1), pl.ds(0, share)], drecv_sem.at[0])
    for mate in mates:
        send(tiles.at[:, my_share], tiles.at[:, my_share], 3, mate)
    for h in range(own_heads):
        columns = block_of(h, me)
        for i, source in enumerate(sources):
            qkv[h, i, my_rows, :] = source[:, columns]
    sides[3].wait()
    arrived(lifts.at[pl.ds(0, pieces)], drecv_sem.at[1])
    arrived(biases.at[pl.ds(0, pieces)], drecv_sem.at[2])
    arrived(tiles.at[:, pl.ds(0, pieces * share)], drecv_sem.at[3])

    frames, reach, columns_here, channels = act1.shape
    own = lifts.shape[2]
    margin = reach // 2
    own_lanes = pl.ds(pl.multiple_of(quarter * own, own), own)

    def inside(d):
        row = seq + d
        return jnp.where(jnp.logical_and(row >= 0, row < seq_size), 1.0, 0.0)

    def silu(value):
        return value / (1.0 + jnp.exp(-value))

    def lifted(chosen, weight, bias):
        return lax.dot_general(
            chosen, weight, (((0,), (0,)), ((), ())), preferred_element_type=jnp.float32
        ) + bias

    wide = [tiles[p].astype(jnp.float32) for p in range(seq_size)]
    for d in range(reach):
        picked = jnp.zeros(wide[0].shape, jnp.float32)
        for p in range(seq_size):
            picked = picked + jnp.where(place_ref[p] == seq + d - margin, 1.0, 0.0) * wide[p]
        for f in range(frames):
            chosen = picked[:, f, :].astype(jnp.bfloat16)
            for c in range(pieces + 1):
                active = silu(lifted(chosen, lifts[c], biases[c])) * inside(d - margin)
                act1[f, d, :, c * own:(c + 1) * own] = active.astype(jnp.bfloat16)
            if 1 <= d <= reach - 2:
                feat[f, d - 1] = lifted(chosen, lifts[quarter], biases[quarter])

    def convolve(layer, active, rows_out):
        length = rows_out * columns_here
        for f in range(frames):
            first = True
            for a in range(3):
                if not 0 <= f + a - 1 < frames:
                    continue
                for b in range(3):
                    window = active[f + a - 1, b:b + rows_out].reshape(length, channels)
                    base = 9 * a + 3 * b
                    term = lax.dot_general(
                        window, taps[layer, base:base + 3].reshape(3 * own, channels),
                        (((1,), (1,)), ((), ())), preferred_element_type=jnp.float32,
                    )
                    acc[f, :length, :] = term if first else acc[f, :length, :] + term
                    first = False

    def gathered_columns(f, r):
        lines = slice(r * columns_here, (r + 1) * columns_here)
        at = lax.broadcasted_iota(jnp.int32, (columns_here, own), 0)
        before = pltpu.roll(acc[f, lines, :own], 1, 0)
        after = pltpu.roll(acc[f, lines, 2 * own:], columns_here - 1, 0)
        return (
            acc[f, lines, own:2 * own]
            + jnp.where(at == 0, 0.0, before)
            + jnp.where(at == columns_here - 1, 0.0, after)
        )

    tap_copy.wait()
    convolve(0, act1, reach - 2)
    for f in range(frames):
        for r in range(reach - 2):
            value = feat[f, r] + gathered_columns(f, r)
            feat[f, r] = value
            act2[f, r, :, own_lanes] = (silu(value) * inside(r + 1 - margin)).astype(jnp.bfloat16)
    for mate in mates:
        send(act2.at[:, :, :, own_lanes], act2.at[:, :, :, own_lanes], 4, mate)

    def last_layer():
        arrived(act2.at[:, :, :, pl.ds(0, pieces * own)], drecv_sem.at[4])
        convolve(1, act2, reach - 4)
        for f in range(frames):
            dec_ref[pl.ds(f, own, stride=frames), :] = jnp.transpose(
                feat[f, margin - 1] + gathered_columns(f, 0)
            )

    half = seq_size // 2
    upper = seq // half

    def nearest(step):
        return upper * (seq_size - 1 - step) + (1 - upper) * step

    block = rep_size * rows
    for h in range(own_heads):
        arrived(qkv.at[h, :, pl.ds(0, others * rows), :], recv_sem.at[h])
        out_columns = block_of(h, me)

        def attend(step, carry):
            target = nearest(seq_size - 1 - step)
            here = pl.ds(pl.multiple_of(target * block, block), block)
            scores = lax.dot_general(
                qkv[h, 0, here, :], qkv[h, 1], (((1,), (1,)), ((), ())),
                preferred_element_type=jnp.float32,
            ) * factor
            exponent = jnp.exp(scores - jnp.max(scores, axis=1, keepdims=True))
            total = jnp.sum(exponent, axis=1, keepdims=True)
            summed = jnp.dot(
                exponent.astype(jnp.bfloat16), qkv[h, 2], preferred_element_type=jnp.float32
            )
            obuf[h, here, :] = (summed / total).astype(jnp.bfloat16)
            for r in range(rep_size):
                @pl.when(jnp.logical_or(target != seq, rep != r))
                def _():
                    start = pl.multiple_of(target * block + r * rows, rows)
                    pltpu.make_async_remote_copy(
                        src_ref=obuf.at[h, pl.ds(start, rows), :],
                        dst_ref=att.at[:, out_columns],
                        send_sem=osend_sem,
                        recv_sem=orecv_sem.at[h * count + me],
                        device_id={"seq": target, "rep": r},
                        device_id_type=MESH,
                    ).start()
            return carry

        lax.fori_loop(0, seq_size, attend, 0)
        att[:, out_columns] = obuf[h, my_rows, :]
        if h == 0:
            last_layer()

    for side in sides[4:]:
        side.wait()
    latent = lat_ref.shape[0]
    squares = jnp.zeros((rows, HEAD_DIM), jnp.float32)
    projected = jnp.zeros((latent, rows), jnp.float32)
    for h in range(own_heads):
        for step in range(seq_size):
            for r in range(rep_size):
                origin = nearest(step) * rep_size + r

                @pl.when(origin != me)
                def _():
                    arrived(obuf.at[h, pl.ds(0, rows), :], orecv_sem.at[h * count + origin])

                cols = block_of(h, origin)
                combined = (
                    stream_ref[:, cols].astype(jnp.float32) + att[:, cols].astype(jnp.float32)
                )
                hidden = combined.astype(jnp.bfloat16)
                hid_ref[:, cols] = hidden
                widened = hidden.astype(jnp.float32)
                squares = squares + widened * widened
                scaled = (widened * gain_ref[:, cols]).astype(jnp.bfloat16)
                projected = projected + lax.dot_general(
                    lw_ref[:, cols], scaled, (((1,), (1,)), ((), ())),
                    preferred_element_type=jnp.float32,
                )
    summed = jnp.sum(jnp.transpose(squares), axis=0, keepdims=True)
    part[:latent] = projected.astype(jnp.bfloat16)
    part[latent:] = jnp.broadcast_to(summed, (part.shape[0] - latent, rows)).astype(jnp.bfloat16)
    swap = pltpu.make_async_remote_copy(
        src_ref=part, dst_ref=part_in, send_sem=psend_sem, recv_sem=precv_sem,
        device_id={"head": lax.rem(head + 1, head_size)}, device_id_type=MESH,
    )
    swap.start()
    arrived(qkv.at[:, :, pl.ds(0, others * rows), :], send_sem)
    arrived(obuf.at[:, pl.ds(0, others * rows), :], osend_sem)
    arrived(tiles.at[pl.ds(0, seq_size - 1), pl.ds(0, share)], dsend_sem.at[0])
    arrived(lifts.at[pl.ds(0, pieces)], dsend_sem.at[1])
    arrived(biases.at[pl.ds(0, pieces)], dsend_sem.at[2])
    arrived(tiles.at[:, pl.ds(0, pieces * share)], dsend_sem.at[3])
    arrived(act2.at[:, :, :, pl.ds(0, pieces * own)], dsend_sem.at[4])
    swap.wait()
    both = part[...].astype(jnp.float32) + part_in[...].astype(jnp.float32)
    lat_ref[...] = both[:latent] * lax.rsqrt(both[latent:latent + 1] / full_width + epsilon)


def finish_kernel(hid_in, lat_in, dec_in, hid_out, lat_out, dec_out, sem):
    writes = [
        pltpu.make_async_copy(held, out, sem.at[i])
        for i, (held, out) in enumerate(
            ((hid_in, hid_out), (lat_in, lat_out), (dec_in, dec_out))
        )
    ]
    for write in writes:
        write.start()
    for write in writes:
        write.wait()


def fused(
    queries, key_tokens, value_tokens, stream, norm_gain, latent_weight,
    tile_pool, tile_position, lift_weight, lift_bias, conv_weight,
):
    seq_size, rep_size, head_size = (lax.axis_size(a) for a in ("seq", "rep", "head"))
    rows, width = queries.shape
    count = seq_size * rep_size
    own_heads = width // HEAD_DIM // count
    latent = latent_weight.shape[1]
    depth, frames, columns = tile_pool.shape[1:]
    layers, _, own, channels = conv_weight.shape
    quarters = head_size * rep_size
    reach = 2 * layers + 1
    bf = jnp.bfloat16
    vmem = pl.BlockSpec(memory_space=pltpu.VMEM)
    hbm = pl.BlockSpec(memory_space=pltpu.HBM)
    dma = pltpu.SemaphoreType.DMA
    held = (
        pltpu.VMEM((rows, width), bf),
        pltpu.VMEM((latent, rows), jnp.float32),
        pltpu.VMEM((own * frames, columns), jnp.float32),
    )
    hidden, latents, decoded = pl.pallas_call(
        functools.partial(fused_kernel, seq_size, rep_size, head_size, width * head_size),
        out_shape=held,
        in_specs=[hbm] * 11,
        out_specs=(vmem, vmem, vmem),
        scratch_shapes=[pltpu.VMEM((rows, width), bf)] * 4 + [
            pltpu.VMEM((1, width), jnp.float32),
            pltpu.VMEM((latent, width), bf),
            pltpu.SMEM(tile_position.shape, jnp.int32),
            pltpu.VMEM((own_heads, 3, count * rows, HEAD_DIM), bf),
            pltpu.VMEM((own_heads, count * rows, HEAD_DIM), bf),
            pltpu.VMEM((rows, width), bf),
            pltpu.VMEM((latent + 16, rows), bf),
            pltpu.VMEM((latent + 16, rows), bf),
            pltpu.VMEM((seq_size, depth, frames, columns), bf),
            pltpu.VMEM((quarters, depth, own), bf),
            pltpu.VMEM((quarters, 1, own), jnp.float32),
            pltpu.VMEM(conv_weight.shape, bf),
            pltpu.VMEM((frames, reach, columns, channels), bf),
            pltpu.VMEM((frames, reach - 2, columns, channels), bf),
            pltpu.VMEM((frames, reach - 2, columns, own), jnp.float32),
            pltpu.VMEM((frames, (reach - 2) * columns, 3 * own), jnp.float32),
            pltpu.SemaphoreType.REGULAR((seq_size - 1,)),
            pltpu.SemaphoreType.REGULAR((head_size - 1,)),
            dma, dma((own_heads,)), dma, dma((own_heads * count,)), dma, dma,
            dma((3 * own_heads,)), dma((7,)), dma, dma((5,)), dma((5,)),
        ],
        compiler_params=pltpu.CompilerParams(
            collective_id=0, has_side_effects=True, vmem_limit_bytes=48 << 20
        ),
    )(*(
        pltpu.with_memory_space_constraint(operand, pltpu.HBM) for operand in (
            queries, key_tokens, value_tokens, stream, norm_gain[None, :], latent_weight.T,
            tile_pool, tile_position, lift_weight, lift_bias[None, :], conv_weight,
        )
    ))
    hidden, latents, decoded = pl.pallas_call(
        finish_kernel,
        out_shape=tuple(jax.ShapeDtypeStruct(ref.shape, ref.dtype) for ref in held),
        in_specs=[vmem, vmem, vmem],
        out_specs=(hbm, hbm, hbm),
        scratch_shapes=[dma((3,))],
        compiler_params=pltpu.CompilerParams(vmem_limit_bytes=8 << 20),
    )(hidden, latents, decoded)
    return hidden, latents.T, decoded.reshape(own, frames, 1, columns)


def gathered(queries, key_tokens, value_tokens, stream, norm_gain, latent_weight):
    query_heads, initial = prepare(queries)
    state = make_update(
        query_heads,
        initial,
        (
            lax.all_gather(key_tokens, ("seq", "rep"), axis=0, tiled=True),
            lax.all_gather(value_tokens, ("seq", "rep"), axis=0, tiled=True),
        ),
    )
    attended = finish(state)
    combined = stream.astype(jnp.float32) + attended.astype(jnp.float32)
    hidden = combined.astype(jnp.bfloat16)
    widened = hidden.astype(jnp.float32)
    scaled = (widened * norm_gain).astype(jnp.bfloat16)
    partial_proj = jnp.dot(scaled, latent_weight, preferred_element_type=jnp.float32)
    partial_squares = jnp.sum(widened * widened, axis=1)
    projected, squares = (
        lax.psum(partial_proj.astype(jnp.bfloat16), "head").astype(jnp.float32),
        lax.psum(partial_squares.astype(jnp.bfloat16), "head").astype(jnp.float32),
    )
    latents = projected * lax.rsqrt(squares / WIDTH + epsilon)[:, None]
    return hidden, latents


def shards(
    queries,
    key_tokens,
    value_tokens,
    stream,
    norm_gain,
    latent_weight,
    tile_pool,
    tile_position,
    lift_weight,
    lift_bias,
    conv_weight,
):
    heads_here = queries.shape[1] // HEAD_DIM
    spread = lax.axis_size("seq") * lax.axis_size("rep")
    fits = heads_here % spread == 0 and lax.axis_size("seq") == 4 and lax.axis_size("head") == 2
    fits = fits and lax.axis_size("rep") == 2 and tile_pool.shape[0] == 1
    fits = fits and conv_weight.shape[0] == 2 and lift_weight.shape[0] % 64 == 0
    if fits:
        return fused(
            queries, key_tokens, value_tokens, stream, norm_gain, latent_weight,
            tile_pool, tile_position, lift_weight, lift_bias, conv_weight,
        )
    hidden, latents = gathered(
        queries, key_tokens, value_tokens, stream, norm_gain, latent_weight
    )
    tiles_here = tile_pool.shape[0]
    frames = tile_pool.shape[2]
    columns = tile_pool.shape[3]
    own_rows = lax.axis_index("seq") * tiles_here + jnp.arange(tiles_here, dtype=jnp.int32)
    collected = make_pick(
        tile_position, own_rows, lax.all_gather(tile_pool, "seq", axis=0, tiled=True)
    )
    latent_grid = collected.astype(jnp.bfloat16)
    channels_here = lift_weight.shape[1]
    feature_map = (
        lax.dot_general(
            lift_weight,
            latent_grid.reshape(latent_grid.shape[0], -1),
            (((0,), (0,)), ((), ())),
            preferred_element_type=jnp.float32,
        )
        + lift_bias[:, None]
    )
    for layer_index in range(conv_weight.shape[0]):
        layer_weight = conv_weight[layer_index]
        active = (
            jax.nn.silu(feature_map)
            .astype(jnp.bfloat16)
            .reshape(channels_here, frames, tiles_here, columns)
        )
        zeros_here = jnp.zeros(feature_map.shape, jnp.float32)
        bordered = padded(active, (("seq", 2),), 1)
        rimmed = lax.all_gather(bordered, ("head", "rep"), axis=0, tiled=True)
        update = tap_sum(zeros_here, rimmed, layer_weight)
        feature_map = feature_map + update
    decoded = feature_map.reshape(channels_here, frames, tiles_here, columns)
    return (hidden, latents, decoded)


def solution(mesh):
    in_specs = (
        P(("groups", "seq", "rep"), "head"),
        P(("groups", "seq", "rep"), "head"),
        P(("groups", "seq", "rep"), "head"),
        P(("groups", "seq", "rep"), "head"),
        P("head"),
        P("head", None),
        P(("groups", "seq"), None, None, None),
        P("groups"),
        P(None, ("head", "rep")),
        P(("head", "rep")),
        P(None, None, ("head", "rep"), None),
    )
    out_specs = (
        P(("groups", "seq", "rep"), "head"),
        P(("groups", "seq", "rep"), None),
        P(("groups", "head", "rep"), None, "seq", None),
    )
    return jax.shard_map(shards, mesh=mesh, in_specs=in_specs, out_specs=out_specs, check_vma=False)
```

```python
import functools
import math

import jax
import jax.numpy as jnp
from jax import lax
from jax.experimental import pallas as pl
from jax.experimental.pallas import tpu as pltpu
from jax.sharding import PartitionSpec as P

HEAD_DIM = 128
WIDTH = 6144


epsilon = 1e-06
negative = -1e30


def padded(shard, sides, width):
    for axis, dim in sides:
        peers, length = (lax.axis_size(axis), shard.shape[dim])
        up = [(i, (i + 1) % peers) for i in range(peers - 1)]
        down = [(j, i) for i, j in up]
        last = lax.slice_in_dim(shard, length - width, length, axis=dim)
        leading = lax.slice_in_dim(shard, 0, width, axis=dim)
        before = lax.ppermute(last, axis, up)
        after = lax.ppermute(leading, axis, down)
        shard = jnp.concatenate([before, shard, after], axis=dim)
    return shard


def prepare(block_rows):
    row_count = block_rows.shape[0]
    head_count = block_rows.shape[1] // HEAD_DIM
    query_heads = block_rows.reshape(row_count, head_count, HEAD_DIM)
    initial = (
        jnp.full((head_count, row_count), negative, jnp.float32),
        jnp.zeros((head_count, row_count), jnp.float32),
        jnp.zeros((head_count, row_count, HEAD_DIM), jnp.float32),
    )
    return (query_heads, initial)


def make_update(query_heads, state, pieces):
    head_count = query_heads.shape[1]
    factor = 1.0 / math.sqrt(HEAD_DIM)
    running_max, running_sum, accum = state
    key_piece, value_piece = pieces
    piece_rows = key_piece.shape[0]
    key_heads = key_piece.reshape(piece_rows, head_count, HEAD_DIM)
    value_heads = value_piece.reshape(piece_rows, head_count, HEAD_DIM)
    scores = (
        jnp.einsum("qhd,khd->hqk", query_heads, key_heads, preferred_element_type=jnp.float32)
        * factor
    )
    new_max = jnp.maximum(running_max, jnp.max(scores, axis=2))
    exponent = jnp.exp(scores - new_max[:, :, None])
    running_sum = jnp.sum(exponent, axis=2)
    accum = jnp.einsum(
        "hqk,khd->hqd",
        exponent.astype(jnp.bfloat16),
        value_heads,
        preferred_element_type=jnp.float32,
    )
    return (new_max, running_sum, accum)


def finish(state):
    running_max, running_sum, accum = state
    result = accum / running_sum[:, :, None]
    return jnp.transpose(result, (1, 0, 2)).reshape(result.shape[1], -1).astype(jnp.bfloat16)


def shift_columns(window, col_shift):
    if col_shift == 0:
        return window
    edge = jnp.zeros(window.shape[:-1] + (1,), window.dtype)
    if col_shift < 0:
        return jnp.concatenate([edge, window[..., :-1]], axis=-1)
    return jnp.concatenate([window[..., 1:], edge], axis=-1)


def tap_sum(running, piece_block, layer_weight):
    piece_rows = piece_block.shape[0]
    frames = piece_block.shape[1]
    band_rows = piece_block.shape[2] - 2
    framed = jnp.pad(piece_block, ((0, 0), (1, 1), (0, 0), (0, 0)))
    for frame_off in range(3):
        for row_off in range(3):
            for col_off in range(3):
                window = shift_columns(
                    framed[:, frame_off : frame_off + frames, row_off : row_off + band_rows, :],
                    col_off - 1,
                )
                tap_weight = layer_weight[frame_off * 9 + row_off * 3 + col_off]
                running = running + lax.dot_general(
                    tap_weight,
                    window.reshape(piece_rows, -1),
                    (((1,), (0,)), ((), ())),
                    preferred_element_type=jnp.float32,
                )
    return running


def make_pick(tile_position, own_rows, piece_block):
    selector = (own_rows[:, None] == tile_position[None, :]).astype(jnp.bfloat16)
    return jnp.einsum("tp,plfc->lftc", selector, piece_block, preferred_element_type=jnp.float32)


MESH = pl.DeviceIdType.MESH


def fused_kernel(
    seq_size, rep_size, head_size, full_width,
    q_hbm, k_hbm, v_hbm, stream_hbm, gain_hbm, lw_hbm,
    tile_hbm, place_hbm, lift_hbm, bias_hbm, conv_hbm,
    hid_ref, lat_ref, dec_ref,
    q_ref, k_ref, v_ref, stream_ref, gain_ref, lw_ref, place_ref,
    qkv, obuf, att, part, part_in,
    tiles, lifts, biases, taps, act1, act2, feat, acc,
    ready, ready_mate,
    send_sem, recv_sem, osend_sem, orecv_sem, psend_sem, precv_sem,
    load_sem, side_sem, tap_sem, dsend_sem, drecv_sem,
):
    seq, rep, head = (lax.axis_index(a) for a in ("seq", "rep", "head"))
    count = seq_size * rep_size
    me = seq * rep_size + rep
    rows = q_ref.shape[0]
    own_heads = qkv.shape[0]
    others = count - 1
    factor = 1.0 / math.sqrt(HEAD_DIM)
    quarter = head * rep_size + rep
    sources = (q_ref, k_ref, v_ref)

    stretch = count * HEAD_DIM
    loads = []
    for h in range(own_heads):
        cols = pl.ds(h * stretch, stretch)
        loads.append([
            pltpu.make_async_copy(origin.at[:, cols], source.at[:, cols], load_sem.at[3 * h + i])
            for i, (origin, source) in enumerate(zip((q_hbm, k_hbm, v_hbm), sources))
        ])
    for load in loads[0]:
        load.start()

    barrier = pltpu.get_barrier_semaphore()
    for e in range(1, rep_size):
        pl.semaphore_signal(
            barrier, inc=1, device_id={"rep": lax.rem(rep + e, rep_size)}, device_id_type=MESH
        )
    for k in range(1, seq_size):
        @pl.when(seq + k < seq_size)
        def _():
            for r in range(rep_size):
                pl.semaphore_signal(
                    barrier, inc=1, device_id={"seq": seq + k, "rep": r}, device_id_type=MESH
                )
    for k in range(1, head_size):
        @pl.when(head + k < head_size)
        def _():
            for r in range(rep_size):
                pl.semaphore_signal(
                    barrier, inc=1, device_id={"head": head + k, "rep": r}, device_id_type=MESH
                )
    pl.semaphore_wait(barrier, rep_size - 1 + rep_size * (seq + head))
    for k in range(1, seq_size):
        @pl.when(seq >= k)
        def _():
            for r in range(rep_size):
                pl.semaphore_signal(
                    ready.at[k - 1], inc=1, device_id={"seq": seq - k, "rep": r},
                    device_id_type=MESH,
                )
    for k in range(1, head_size):
        @pl.when(head >= k)
        def _():
            for r in range(rep_size):
                pl.semaphore_signal(
                    ready_mate.at[k - 1], inc=1, device_id={"head": head - k, "rep": r},
                    device_id_type=MESH,
                )

    half = seq_size // 2
    upper = seq // half
    far = (1 - upper) * half
    inner = upper * half + (1 - upper) * (half - 1)
    mirror = 2 * half * upper + half - 1 - seq
    share = tiles.shape[1] // rep_size
    my_share = pl.ds(pl.multiple_of(rep * share, share), share)
    sides = [
        pltpu.make_async_copy(origin, target, side_sem.at[i])
        for i, (origin, target) in enumerate((
            (tile_hbm.at[0, my_share], tiles.at[seq, my_share]),
            (lift_hbm, lifts.at[quarter]),
            (bias_hbm, biases.at[quarter]),
            (place_hbm, place_ref),
            (stream_hbm, stream_ref),
            (gain_hbm, gain_ref),
            (lw_hbm, lw_ref),
        ))
    ]
    @pl.when(head == 0)
    def _():
        sides[0].start()


    def arrived(ref, sem):
        pltpu.make_async_copy(ref, ref, sem).wait()

    def send(source, target, index, device):
        pltpu.make_async_remote_copy(
            src_ref=source, dst_ref=target,
            send_sem=dsend_sem.at[index], recv_sem=drecv_sem.at[index],
            device_id=device, device_id_type=MESH,
        ).start()

    my_rows = pl.ds(pl.multiple_of(me * rows, rows), rows)

    def block_of(h, place):
        return pl.ds(pl.multiple_of((h * count + place) * HEAD_DIM, HEAD_DIM), HEAD_DIM)

    def send_one(h, i, target, r):
        pltpu.make_async_remote_copy(
            src_ref=sources[i].at[:, block_of(h, target * rep_size + r)],
            dst_ref=qkv.at[h, i, my_rows, :],
            send_sem=send_sem,
            recv_sem=recv_sem.at[h],
            device_id={"seq": target, "rep": r},
            device_id_type=MESH,
        ).start()

    def send_back(h, arrays):
        for k in (2, 1, 3):
            @pl.when(seq >= k)
            def _():
                for r in range(rep_size):
                    for i in arrays:
                        send_one(h, i, seq - k, r)

    def send_on(h):
        for k in range(1, seq_size):
            @pl.when(seq + k < seq_size)
            def _():
                if h == 0:
                    pl.semaphore_wait(ready.at[k - 1], rep_size)
                for r in range(rep_size):
                    for i in range(3):
                        send_one(h, i, seq + k, r)
        for e in range(1, rep_size):
            for i in range(3):
                send_one(h, i, seq, lax.rem(rep + e, rep_size))

    own_tile = tiles.at[seq, my_share]
    far_tiles = tiles.at[pl.ds(far, half), my_share]
    for i, load in enumerate(loads[0]):
        load.wait()
        send_back(0, (i,))
    for pending in loads[1:]:
        for load in pending:
            load.start()
    send_on(0)

    @pl.when(head == 0)
    def _():
        sides[0].wait()
        send(own_tile, own_tile, 0, {"seq": mirror})
        send(own_tile, own_tile, 0, {"seq": (1 - upper) * half + upper * (half - 1)})

        @pl.when(seq == inner)
        def _():
            arrived(tiles.at[pl.ds(0, seq_size - 1), pl.ds(0, share)], drecv_sem.at[0])
            pltpu.make_async_remote_copy(
                src_ref=far_tiles, dst_ref=far_tiles,
                send_sem=dsend_sem.at[5], recv_sem=drecv_sem.at[0],
                device_id={"seq": mirror}, device_id_type=MESH,
            ).start()

    tap_copy = pltpu.make_async_copy(conv_hbm, taps, tap_sem)
    tap_copy.start()
    for side in sides[1:]:
        side.start()
    for h in range(1, own_heads):
        for load in loads[h]:
            load.wait()
        send_back(h, range(3))
        send_on(h)

    mates = [
        {"head": lax.rem(head + d, head_size), "rep": lax.rem(rep + e, rep_size)}
        for d in range(head_size) for e in range(rep_size) if (d, e) != (0, 0)
    ]
    for k in range(1, head_size):
        @pl.when(head + k < head_size)
        def _():
            pl.semaphore_wait(ready_mate.at[k - 1], rep_size)
    sides[1].wait()
    sides[2].wait()
    for mate in mates:
        send(lifts.at[quarter], lifts.at[quarter], 1, mate)
        send(biases.at[quarter], biases.at[quarter], 2, mate)
    pieces = len(mates)
    @pl.when(head == 0)
    def _():
        @pl.when(seq != inner)
        def _():
            arrived(tiles.at[pl.ds(0, seq_size - 1), pl.ds(0, share)], drecv_sem.at[0])

        for mate in mates:
            send(tiles.at[:, my_share], tiles.at[:, my_share], 3, mate)

    for h in range(own_heads):
        columns = block_of(h, me)
        for i, source in enumerate(sources):
            qkv[h, i, my_rows, :] = source[:, columns]
    sides[3].wait()
    arrived(lifts.at[pl.ds(0, pieces)], drecv_sem.at[1])
    arrived(biases.at[pl.ds(0, pieces)], drecv_sem.at[2])
    @pl.when(head == 0)
    def _():
        arrived(tiles.at[:, pl.ds(0, (rep_size - 1) * share)], drecv_sem.at[3])

    @pl.when(head != 0)
    def _():
        arrived(tiles, drecv_sem.at[3])

    frames, reach, columns_here, channels = act1.shape
    own = lifts.shape[2]
    margin = reach // 2
    own_lanes = pl.ds(pl.multiple_of(quarter * own, own), own)

    def inside(d):
        row = seq + d
        return jnp.where(jnp.logical_and(row >= 0, row < seq_size), 1.0, 0.0)

    def silu(value):
        return value / (1.0 + jnp.exp(-value))

    def lifted(chosen, weight, bias):
        return lax.dot_general(
            chosen, weight, (((0,), (0,)), ((), ())), preferred_element_type=jnp.float32
        ) + bias

    wide = [tiles[p].astype(jnp.float32) for p in range(seq_size)]
    for d in range(reach):
        picked = jnp.zeros(wide[0].shape, jnp.float32)
        for p in range(seq_size):
            picked = picked + jnp.where(place_ref[p] == seq + d - margin, 1.0, 0.0) * wide[p]
        for f in range(frames):
            chosen = picked[:, f, :].astype(jnp.bfloat16)
            for c in range(pieces + 1):
                active = silu(lifted(chosen, lifts[c], biases[c])) * inside(d - margin)
                act1[f, d, :, c * own:(c + 1) * own] = active.astype(jnp.bfloat16)
            if 1 <= d <= reach - 2:
                feat[f, d - 1] = lifted(chosen, lifts[quarter], biases[quarter])

    def convolve(layer, active, rows_out):
        length = rows_out * columns_here
        for f in range(frames):
            first = True
            for a in range(3):
                if not 0 <= f + a - 1 < frames:
                    continue
                for b in range(3):
                    window = active[f + a - 1, b:b + rows_out].reshape(length, channels)
                    base = 9 * a + 3 * b
                    term = lax.dot_general(
                        window, taps[layer, base:base + 3].reshape(3 * own, channels),
                        (((1,), (1,)), ((), ())), preferred_element_type=jnp.float32,
                    )
                    acc[f, :length, :] = term if first else acc[f, :length, :] + term
                    first = False

    def gathered_columns(f, r):
        lines = slice(r * columns_here, (r + 1) * columns_here)
        at = lax.broadcasted_iota(jnp.int32, (columns_here, own), 0)
        before = pltpu.roll(acc[f, lines, :own], 1, 0)
        after = pltpu.roll(acc[f, lines, 2 * own:], columns_here - 1, 0)
        return (
            acc[f, lines, own:2 * own]
            + jnp.where(at == 0, 0.0, before)
            + jnp.where(at == columns_here - 1, 0.0, after)
        )

    tap_copy.wait()
    convolve(0, act1, reach - 2)
    for f in range(frames):
        for r in range(reach - 2):
            value = feat[f, r] + gathered_columns(f, r)
            feat[f, r] = value
            act2[f, r, :, own_lanes] = (silu(value) * inside(r + 1 - margin)).astype(jnp.bfloat16)
    for mate in mates:
        send(act2.at[:, :, :, own_lanes], act2.at[:, :, :, own_lanes], 4, mate)

    def last_layer():
        arrived(act2.at[:, :, :, pl.ds(0, pieces * own)], drecv_sem.at[4])
        convolve(1, act2, reach - 4)
        for f in range(frames):
            dec_ref[pl.ds(f, own, stride=frames), :] = jnp.transpose(
                feat[f, margin - 1] + gathered_columns(f, 0)
            )

    def give(h, target, r):
        start = pl.multiple_of(target * block + r * rows, rows)
        pltpu.make_async_remote_copy(
            src_ref=obuf.at[h, pl.ds(start, rows), :],
            dst_ref=att.at[:, block_of(h, me)],
            send_sem=osend_sem,
            recv_sem=orecv_sem.at[h * count + me],
            device_id={"seq": target, "rep": r},
            device_id_type=MESH,
        ).start()

    block = rep_size * rows
    for h in range(own_heads):
        arrived(qkv.at[h, :, pl.ds(0, others * rows), :], recv_sem.at[h])

        def attend(step, carry):
            target = lax.rem(far + step, seq_size)
            here = pl.ds(pl.multiple_of(target * block, block), block)
            scores = lax.dot_general(
                qkv[h, 0, here, :], qkv[h, 1], (((1,), (1,)), ((), ())),
                preferred_element_type=jnp.float32,
            ) * factor
            exponent = jnp.exp(scores - jnp.max(scores, axis=1, keepdims=True))
            total = jnp.sum(exponent, axis=1, keepdims=True)
            summed = jnp.dot(
                exponent.astype(jnp.bfloat16), qkv[h, 2], preferred_element_type=jnp.float32
            )
            obuf[h, here, :] = (summed / total).astype(jnp.bfloat16)
            for r in range(rep_size):
                other = jnp.logical_or(target != seq, rep != r)
                if r == rep_size - 1:
                    if h < own_heads - 1:
                        other = jnp.logical_and(other, step != 1)
                    else:
                        @pl.when(step == 1)
                        def _():
                            for e in range(own_heads - 1):
                                give(e, target, r)

                @pl.when(other)
                def _():
                    give(h, target, r)
            return carry

        lax.fori_loop(0, seq_size, attend, 0)
        att[:, block_of(h, me)] = obuf[h, my_rows, :]
        if h == 0:
            last_layer()

    for side in sides[4:]:
        side.wait()
    latent = lat_ref.shape[0]
    squares = jnp.zeros((rows, HEAD_DIM), jnp.float32)
    projected = jnp.zeros((latent, rows), jnp.float32)
    for h, step in [
        (h, half * across + step)
        for across in (1, 0) for h in range(own_heads) for step in range(half)
    ]:
        for r in range(rep_size):
            origin = lax.rem(far + step, seq_size) * rep_size + r

            @pl.when(origin != me)
            def _():
                arrived(obuf.at[h, pl.ds(0, rows), :], orecv_sem.at[h * count + origin])

            cols = block_of(h, origin)
            combined = (
                stream_ref[:, cols].astype(jnp.float32) + att[:, cols].astype(jnp.float32)
            )
            hidden = combined.astype(jnp.bfloat16)
            hid_ref[:, cols] = hidden
            widened = hidden.astype(jnp.float32)
            squares = squares + widened * widened
            scaled = (widened * gain_ref[:, cols]).astype(jnp.bfloat16)
            projected = projected + lax.dot_general(
                lw_ref[:, cols], scaled, (((1,), (1,)), ((), ())),
                preferred_element_type=jnp.float32,
            )
    summed = jnp.sum(jnp.transpose(squares), axis=0, keepdims=True)
    part[:latent] = projected.astype(jnp.bfloat16)
    part[latent:] = jnp.broadcast_to(summed, (part.shape[0] - latent, rows)).astype(jnp.bfloat16)
    swap = pltpu.make_async_remote_copy(
        src_ref=part, dst_ref=part_in, send_sem=psend_sem, recv_sem=precv_sem,
        device_id={"head": lax.rem(head + 1, head_size)}, device_id_type=MESH,
    )
    swap.start()
    arrived(qkv.at[:, :, pl.ds(0, others * rows), :], send_sem)
    arrived(obuf.at[:, pl.ds(0, others * rows), :], osend_sem)
    arrived(lifts.at[pl.ds(0, pieces)], dsend_sem.at[1])
    arrived(biases.at[pl.ds(0, pieces)], dsend_sem.at[2])

    @pl.when(head == 0)
    def _():
        arrived(tiles.at[pl.ds(0, 2), pl.ds(0, share)], dsend_sem.at[0])
        told = pieces * seq_size * share * frames * columns_here // HEAD_DIM
        arrived(obuf.at[0, pl.ds(0, told), :], dsend_sem.at[3])

        @pl.when(seq == inner)
        def _():
            arrived(far_tiles, dsend_sem.at[5])

    arrived(act2.at[:, :, :, pl.ds(0, pieces * own)], dsend_sem.at[4])
    swap.wait()
    both = part[...].astype(jnp.float32) + part_in[...].astype(jnp.float32)
    lat_ref[...] = both[:latent] * lax.rsqrt(both[latent:latent + 1] / full_width + epsilon)


def finish_kernel(hid_in, lat_in, dec_in, hid_out, lat_out, dec_out, sem):
    writes = [
        pltpu.make_async_copy(held, out, sem.at[i])
        for i, (held, out) in enumerate(
            ((hid_in, hid_out), (lat_in, lat_out), (dec_in, dec_out))
        )
    ]
    for write in writes:
        write.start()
    for write in writes:
        write.wait()


def fused(
    queries, key_tokens, value_tokens, stream, norm_gain, latent_weight,
    tile_pool, tile_position, lift_weight, lift_bias, conv_weight,
):
    seq_size, rep_size, head_size = (lax.axis_size(a) for a in ("seq", "rep", "head"))
    rows, width = queries.shape
    count = seq_size * rep_size
    own_heads = width // HEAD_DIM // count
    latent = latent_weight.shape[1]
    depth, frames, columns = tile_pool.shape[1:]
    layers, _, own, channels = conv_weight.shape
    quarters = head_size * rep_size
    reach = 2 * layers + 1
    bf = jnp.bfloat16
    vmem = pl.BlockSpec(memory_space=pltpu.VMEM)
    hbm = pl.BlockSpec(memory_space=pltpu.HBM)
    dma = pltpu.SemaphoreType.DMA
    held = (
        pltpu.VMEM((rows, width), bf),
        pltpu.VMEM((latent, rows), jnp.float32),
        pltpu.VMEM((own * frames, columns), jnp.float32),
    )
    hidden, latents, decoded = pl.pallas_call(
        functools.partial(fused_kernel, seq_size, rep_size, head_size, width * head_size),
        out_shape=held,
        in_specs=[hbm] * 11,
        out_specs=(vmem, vmem, vmem),
        scratch_shapes=[pltpu.VMEM((rows, width), bf)] * 4 + [
            pltpu.VMEM((1, width), jnp.float32),
            pltpu.VMEM((latent, width), bf),
            pltpu.SMEM(tile_position.shape, jnp.int32),
            pltpu.VMEM((own_heads, 3, count * rows, HEAD_DIM), bf),
            pltpu.VMEM((own_heads, count * rows, HEAD_DIM), bf),
            pltpu.VMEM((rows, width), bf),
            pltpu.VMEM((latent + 16, rows), bf),
            pltpu.VMEM((latent + 16, rows), bf),
            pltpu.VMEM((seq_size, depth, frames, columns), bf),
            pltpu.VMEM((quarters, depth, own), bf),
            pltpu.VMEM((quarters, 1, own), jnp.float32),
            pltpu.VMEM(conv_weight.shape, bf),
            pltpu.VMEM((frames, reach, columns, channels), bf),
            pltpu.VMEM((frames, reach - 2, columns, channels), bf),
            pltpu.VMEM((frames, reach - 2, columns, own), jnp.float32),
            pltpu.VMEM((frames, (reach - 2) * columns, 3 * own), jnp.float32),
            pltpu.SemaphoreType.REGULAR((seq_size - 1,)),
            pltpu.SemaphoreType.REGULAR((head_size - 1,)),
            dma, dma((own_heads,)), dma, dma((own_heads * count,)), dma, dma,
            dma((3 * own_heads,)), dma((7,)), dma, dma((6,)), dma((5,)),
        ],
        compiler_params=pltpu.CompilerParams(
            collective_id=0, has_side_effects=True, vmem_limit_bytes=48 << 20
        ),
    )(*(
        pltpu.with_memory_space_constraint(operand, pltpu.HBM) for operand in (
            queries, key_tokens, value_tokens, stream, norm_gain[None, :], latent_weight.T,
            tile_pool, tile_position, lift_weight, lift_bias[None, :], conv_weight,
        )
    ))
    hidden, latents, decoded = pl.pallas_call(
        finish_kernel,
        out_shape=tuple(jax.ShapeDtypeStruct(ref.shape, ref.dtype) for ref in held),
        in_specs=[vmem, vmem, vmem],
        out_specs=(hbm, hbm, hbm),
        scratch_shapes=[dma((3,))],
        compiler_params=pltpu.CompilerParams(vmem_limit_bytes=8 << 20),
    )(hidden, latents, decoded)
    return hidden, latents.T, decoded.reshape(own, frames, 1, columns)


def gathered(queries, key_tokens, value_tokens, stream, norm_gain, latent_weight):
    query_heads, initial = prepare(queries)
    state = make_update(
        query_heads,
        initial,
        (
            lax.all_gather(key_tokens, ("seq", "rep"), axis=0, tiled=True),
            lax.all_gather(value_tokens, ("seq", "rep"), axis=0, tiled=True),
        ),
    )
    attended = finish(state)
    combined = stream.astype(jnp.float32) + attended.astype(jnp.float32)
    hidden = combined.astype(jnp.bfloat16)
    widened = hidden.astype(jnp.float32)
    scaled = (widened * norm_gain).astype(jnp.bfloat16)
    partial_proj = jnp.dot(scaled, latent_weight, preferred_element_type=jnp.float32)
    partial_squares = jnp.sum(widened * widened, axis=1)
    projected, squares = (
        lax.psum(partial_proj.astype(jnp.bfloat16), "head").astype(jnp.float32),
        lax.psum(partial_squares.astype(jnp.bfloat16), "head").astype(jnp.float32),
    )
    latents = projected * lax.rsqrt(squares / WIDTH + epsilon)[:, None]
    return hidden, latents


def shards(
    queries,
    key_tokens,
    value_tokens,
    stream,
    norm_gain,
    latent_weight,
    tile_pool,
    tile_position,
    lift_weight,
    lift_bias,
    conv_weight,
):
    heads_here = queries.shape[1] // HEAD_DIM
    spread = lax.axis_size("seq") * lax.axis_size("rep")
    fits = heads_here % spread == 0 and lax.axis_size("seq") == 4 and lax.axis_size("head") == 2
    fits = fits and lax.axis_size("rep") == 2 and tile_pool.shape[0] == 1
    fits = fits and conv_weight.shape[0] == 2 and lift_weight.shape[0] % 64 == 0
    if fits:
        return fused(
            queries, key_tokens, value_tokens, stream, norm_gain, latent_weight,
            tile_pool, tile_position, lift_weight, lift_bias, conv_weight,
        )
    hidden, latents = gathered(
        queries, key_tokens, value_tokens, stream, norm_gain, latent_weight
    )
    tiles_here = tile_pool.shape[0]
    frames = tile_pool.shape[2]
    columns = tile_pool.shape[3]
    own_rows = lax.axis_index("seq") * tiles_here + jnp.arange(tiles_here, dtype=jnp.int32)
    collected = make_pick(
        tile_position, own_rows, lax.all_gather(tile_pool, "seq", axis=0, tiled=True)
    )
    latent_grid = collected.astype(jnp.bfloat16)
    channels_here = lift_weight.shape[1]
    feature_map = (
        lax.dot_general(
            lift_weight,
            latent_grid.reshape(latent_grid.shape[0], -1),
            (((0,), (0,)), ((), ())),
            preferred_element_type=jnp.float32,
        )
        + lift_bias[:, None]
    )
    for layer_index in range(conv_weight.shape[0]):
        layer_weight = conv_weight[layer_index]
        active = (
            jax.nn.silu(feature_map)
            .astype(jnp.bfloat16)
            .reshape(channels_here, frames, tiles_here, columns)
        )
        zeros_here = jnp.zeros(feature_map.shape, jnp.float32)
        bordered = padded(active, (("seq", 2),), 1)
        rimmed = lax.all_gather(bordered, ("head", "rep"), axis=0, tiled=True)
        update = tap_sum(zeros_here, rimmed, layer_weight)
        feature_map = feature_map + update
    decoded = feature_map.reshape(channels_here, frames, tiles_here, columns)
    return (hidden, latents, decoded)


def solution(mesh):
    in_specs = (
        P(("groups", "seq", "rep"), "head"),
        P(("groups", "seq", "rep"), "head"),
        P(("groups", "seq", "rep"), "head"),
        P(("groups", "seq", "rep"), "head"),
        P("head"),
        P("head", None),
        P(("groups", "seq"), None, None, None),
        P("groups"),
        P(None, ("head", "rep")),
        P(("head", "rep")),
        P(None, None, ("head", "rep"), None),
    )
    out_specs = (
        P(("groups", "seq", "rep"), "head"),
        P(("groups", "seq", "rep"), None),
        P(("groups", "head", "rep"), None, "seq", None),
    )
    return jax.shard_map(shards, mesh=mesh, in_specs=in_specs, out_specs=out_specs, check_vma=False)
```

```python
import functools
import math

import jax
import jax.numpy as jnp
from jax import lax
from jax.experimental import pallas as pl
from jax.experimental.pallas import tpu as pltpu
from jax.sharding import PartitionSpec as P

HEAD_DIM = 128
WIDTH = 6144


epsilon = 1e-06
negative = -1e30


def padded(shard, sides, width):
    for axis, dim in sides:
        peers, length = (lax.axis_size(axis), shard.shape[dim])
        up = [(i, (i + 1) % peers) for i in range(peers - 1)]
        down = [(j, i) for i, j in up]
        last = lax.slice_in_dim(shard, length - width, length, axis=dim)
        leading = lax.slice_in_dim(shard, 0, width, axis=dim)
        before = lax.ppermute(last, axis, up)
        after = lax.ppermute(leading, axis, down)
        shard = jnp.concatenate([before, shard, after], axis=dim)
    return shard


def prepare(block_rows):
    row_count = block_rows.shape[0]
    head_count = block_rows.shape[1] // HEAD_DIM
    query_heads = block_rows.reshape(row_count, head_count, HEAD_DIM)
    initial = (
        jnp.full((head_count, row_count), negative, jnp.float32),
        jnp.zeros((head_count, row_count), jnp.float32),
        jnp.zeros((head_count, row_count, HEAD_DIM), jnp.float32),
    )
    return (query_heads, initial)


def make_update(query_heads, state, pieces):
    head_count = query_heads.shape[1]
    factor = 1.0 / math.sqrt(HEAD_DIM)
    running_max, running_sum, accum = state
    key_piece, value_piece = pieces
    piece_rows = key_piece.shape[0]
    key_heads = key_piece.reshape(piece_rows, head_count, HEAD_DIM)
    value_heads = value_piece.reshape(piece_rows, head_count, HEAD_DIM)
    scores = (
        jnp.einsum("qhd,khd->hqk", query_heads, key_heads, preferred_element_type=jnp.float32)
        * factor
    )
    new_max = jnp.maximum(running_max, jnp.max(scores, axis=2))
    exponent = jnp.exp(scores - new_max[:, :, None])
    running_sum = jnp.sum(exponent, axis=2)
    accum = jnp.einsum(
        "hqk,khd->hqd",
        exponent.astype(jnp.bfloat16),
        value_heads,
        preferred_element_type=jnp.float32,
    )
    return (new_max, running_sum, accum)


def finish(state):
    running_max, running_sum, accum = state
    result = accum / running_sum[:, :, None]
    return jnp.transpose(result, (1, 0, 2)).reshape(result.shape[1], -1).astype(jnp.bfloat16)


def shift_columns(window, col_shift):
    if col_shift == 0:
        return window
    edge = jnp.zeros(window.shape[:-1] + (1,), window.dtype)
    if col_shift < 0:
        return jnp.concatenate([edge, window[..., :-1]], axis=-1)
    return jnp.concatenate([window[..., 1:], edge], axis=-1)


def tap_sum(running, piece_block, layer_weight):
    piece_rows = piece_block.shape[0]
    frames = piece_block.shape[1]
    band_rows = piece_block.shape[2] - 2
    framed = jnp.pad(piece_block, ((0, 0), (1, 1), (0, 0), (0, 0)))
    for frame_off in range(3):
        for row_off in range(3):
            for col_off in range(3):
                window = shift_columns(
                    framed[:, frame_off : frame_off + frames, row_off : row_off + band_rows, :],
                    col_off - 1,
                )
                tap_weight = layer_weight[frame_off * 9 + row_off * 3 + col_off]
                running = running + lax.dot_general(
                    tap_weight,
                    window.reshape(piece_rows, -1),
                    (((1,), (0,)), ((), ())),
                    preferred_element_type=jnp.float32,
                )
    return running


def make_pick(tile_position, own_rows, piece_block):
    selector = (own_rows[:, None] == tile_position[None, :]).astype(jnp.bfloat16)
    return jnp.einsum("tp,plfc->lftc", selector, piece_block, preferred_element_type=jnp.float32)


MESH = pl.DeviceIdType.MESH


def fused_kernel(
    seq_size, rep_size, head_size, full_width,
    q_hbm, k_hbm, v_hbm, stream_hbm, gain_hbm, lw_hbm,
    tile_hbm, place_hbm, lift_hbm, bias_hbm, conv_hbm,
    hid_ref, lat_ref, dec_ref,
    q_ref, k_ref, v_ref, stream_ref, gain_ref, lw_ref, place_ref,
    qkv, obuf, att, part, part_in,
    tiles, lifts, biases, taps, act1, act2, feat, acc,
    ready, ready_mate,
    send_sem, recv_sem, osend_sem, orecv_sem, psend_sem, precv_sem,
    load_sem, side_sem, tap_sem, dsend_sem, drecv_sem,
):
    seq, rep, head = (lax.axis_index(a) for a in ("seq", "rep", "head"))
    count = seq_size * rep_size
    me = seq * rep_size + rep
    rows = q_ref.shape[0]
    own_heads = qkv.shape[0]
    others = count - 1
    factor = 1.0 / math.sqrt(HEAD_DIM)
    quarter = head * rep_size + rep
    sources = (q_ref, k_ref, v_ref)

    stretch = count * HEAD_DIM
    loads = []
    for h in range(own_heads):
        cols = pl.ds(h * stretch, stretch)
        loads.append([
            pltpu.make_async_copy(origin.at[:, cols], source.at[:, cols], load_sem.at[3 * h + i])
            for i, (origin, source) in enumerate(zip((q_hbm, k_hbm, v_hbm), sources))
        ])
    for load in loads[0]:
        load.start()

    barrier = pltpu.get_barrier_semaphore()
    for e in range(1, rep_size):
        pl.semaphore_signal(
            barrier, inc=1, device_id={"rep": lax.rem(rep + e, rep_size)}, device_id_type=MESH
        )
    for k in range(1, seq_size):
        @pl.when(seq + k < seq_size)
        def _():
            for r in range(rep_size):
                pl.semaphore_signal(
                    barrier, inc=1, device_id={"seq": seq + k, "rep": r}, device_id_type=MESH
                )
    half = seq_size // 2

    @pl.when(seq == half)
    def _():
        for r in range(rep_size):
            pl.semaphore_signal(
                barrier, inc=1, device_id={"seq": seq - 1, "rep": r}, device_id_type=MESH
            )

    for k in range(1, head_size):
        @pl.when(head + k < head_size)
        def _():
            for r in range(rep_size):
                pl.semaphore_signal(
                    barrier, inc=1, device_id={"head": head + k, "rep": r}, device_id_type=MESH
                )
    greeted = seq + head + jnp.where(seq == half - 1, 1, 0)
    pl.semaphore_wait(barrier, rep_size - 1 + rep_size * greeted)
    for k in range(1, seq_size):
        @pl.when(jnp.logical_and(seq >= k, jnp.logical_or(k > 1, seq != half)))
        def _():
            for r in range(rep_size):
                pl.semaphore_signal(
                    ready.at[k - 1], inc=1, device_id={"seq": seq - k, "rep": r},
                    device_id_type=MESH,
                )
    for k in range(1, head_size):
        @pl.when(head >= k)
        def _():
            for r in range(rep_size):
                pl.semaphore_signal(
                    ready_mate.at[k - 1], inc=1, device_id={"head": head - k, "rep": r},
                    device_id_type=MESH,
                )

    upper = seq // half
    far = (1 - upper) * half
    inner = upper * half + (1 - upper) * (half - 1)
    mirror = 2 * half * upper + half - 1 - seq
    share = tiles.shape[1] // rep_size
    my_share = pl.ds(pl.multiple_of(rep * share, share), share)
    sides = [
        pltpu.make_async_copy(origin, target, side_sem.at[i])
        for i, (origin, target) in enumerate((
            (tile_hbm.at[0, my_share], tiles.at[seq, my_share]),
            (lift_hbm, lifts.at[quarter]),
            (bias_hbm, biases.at[quarter]),
            (place_hbm, place_ref),
            (stream_hbm, stream_ref),
            (gain_hbm, gain_ref),
            (lw_hbm, lw_ref),
        ))
    ]
    @pl.when(head == 0)
    def _():
        sides[0].start()


    def arrived(ref, sem):
        pltpu.make_async_copy(ref, ref, sem).wait()

    def send(source, target, index, device):
        pltpu.make_async_remote_copy(
            src_ref=source, dst_ref=target,
            send_sem=dsend_sem.at[index], recv_sem=drecv_sem.at[index],
            device_id=device, device_id_type=MESH,
        ).start()

    my_rows = pl.ds(pl.multiple_of(me * rows, rows), rows)

    def block_of(h, place):
        return pl.ds(pl.multiple_of((h * count + place) * HEAD_DIM, HEAD_DIM), HEAD_DIM)

    def send_one(h, i, target, r):
        pltpu.make_async_remote_copy(
            src_ref=sources[i].at[:, block_of(h, target * rep_size + r)],
            dst_ref=qkv.at[h, i, my_rows, :],
            send_sem=send_sem,
            recv_sem=recv_sem.at[h],
            device_id={"seq": target, "rep": r},
            device_id_type=MESH,
        ).start()

    def send_back(h, arrays):
        for k in (2, 1, 3):
            @pl.when(seq >= k)
            def _():
                for r in range(rep_size):
                    for i in arrays:
                        send_one(h, i, seq - k, r)

    def send_on(h):
        for k in range(1, seq_size):
            @pl.when(seq + k < seq_size)
            def _():
                if h == 0:
                    @pl.when(jnp.logical_or(k > 1, seq != half - 1))
                    def _():
                        pl.semaphore_wait(ready.at[k - 1], rep_size)

                for r in range(rep_size):
                    for i in range(3):
                        send_one(h, i, seq + k, r)
        for e in range(1, rep_size):
            for i in range(3):
                send_one(h, i, seq, lax.rem(rep + e, rep_size))

    own_tile = tiles.at[seq, my_share]
    far_tiles = tiles.at[pl.ds(far, half), my_share]
    for i, load in enumerate(loads[0]):
        load.wait()
        send_back(0, (i,))
    for pending in loads[1:]:
        for load in pending:
            load.start()
    send_on(0)

    @pl.when(head == 0)
    def _():
        sides[0].wait()
        send(own_tile, own_tile, 0, {"seq": mirror})
        send(own_tile, own_tile, 0, {"seq": (1 - upper) * half + upper * (half - 1)})

    tap_copy = pltpu.make_async_copy(conv_hbm, taps, tap_sem)
    tap_copy.start()
    for side in sides[1:]:
        side.start()
    for h in range(1, own_heads):
        for load in loads[h]:
            load.wait()
        send_back(h, range(3))
        send_on(h)

    @pl.when(head == 0)
    def _():
        @pl.when(seq == inner)
        def _():
            arrived(tiles.at[pl.ds(0, seq_size - 1), pl.ds(0, share)], drecv_sem.at[0])
            pltpu.make_async_remote_copy(
                src_ref=far_tiles, dst_ref=far_tiles,
                send_sem=dsend_sem.at[5], recv_sem=drecv_sem.at[0],
                device_id={"seq": mirror}, device_id_type=MESH,
            ).start()

    mates = [
        {"head": lax.rem(head + d, head_size), "rep": lax.rem(rep + e, rep_size)}
        for d in range(head_size) for e in range(rep_size) if (d, e) != (0, 0)
    ]
    for k in range(1, head_size):
        @pl.when(head + k < head_size)
        def _():
            pl.semaphore_wait(ready_mate.at[k - 1], rep_size)
    sides[1].wait()
    sides[2].wait()
    for mate in mates:
        send(lifts.at[quarter], lifts.at[quarter], 1, mate)
        send(biases.at[quarter], biases.at[quarter], 2, mate)
    pieces = len(mates)
    for h in range(own_heads):
        columns = block_of(h, me)
        for i, source in enumerate(sources):
            qkv[h, i, my_rows, :] = source[:, columns]
    frames, reach, columns_here, channels = act1.shape
    own = lifts.shape[2]
    margin = reach // 2
    own_lanes = pl.ds(pl.multiple_of(quarter * own, own), own)

    def inside(d):
        row = seq + d
        return jnp.where(jnp.logical_and(row >= 0, row < seq_size), 1.0, 0.0)

    def silu(value):
        return value / (1.0 + jnp.exp(-value))

    def lifted(chosen, weight, bias):
        return lax.dot_general(
            chosen, weight, (((0,), (0,)), ((), ())), preferred_element_type=jnp.float32
        ) + bias

    def convolve(layer, active, rows_out):
        length = rows_out * columns_here
        for f in range(frames):
            first = True
            for a in range(3):
                if not 0 <= f + a - 1 < frames:
                    continue
                for b in range(3):
                    window = active[f + a - 1, b:b + rows_out].reshape(length, channels)
                    base = 9 * a + 3 * b
                    term = lax.dot_general(
                        window, taps[layer, base:base + 3].reshape(3 * own, channels),
                        (((1,), (1,)), ((), ())), preferred_element_type=jnp.float32,
                    )
                    acc[f, :length, :] = term if first else acc[f, :length, :] + term
                    first = False

    def gathered_columns(f, r):
        lines = slice(r * columns_here, (r + 1) * columns_here)
        at = lax.broadcasted_iota(jnp.int32, (columns_here, own), 0)
        before = pltpu.roll(acc[f, lines, :own], 1, 0)
        after = pltpu.roll(acc[f, lines, 2 * own:], columns_here - 1, 0)
        return (
            acc[f, lines, own:2 * own]
            + jnp.where(at == 0, 0.0, before)
            + jnp.where(at == columns_here - 1, 0.0, after)
        )

    def first_layer():
        @pl.when(head == 0)
        def _():
            @pl.when(seq != inner)
            def _():
                arrived(tiles.at[pl.ds(0, seq_size - 1), pl.ds(0, share)], drecv_sem.at[0])

            for mate in mates:
                send(tiles.at[:, my_share], tiles.at[:, my_share], 3, mate)

        sides[3].wait()
        arrived(lifts.at[pl.ds(0, pieces)], drecv_sem.at[1])
        arrived(biases.at[pl.ds(0, pieces)], drecv_sem.at[2])
        @pl.when(head == 0)
        def _():
            arrived(tiles.at[:, pl.ds(0, (rep_size - 1) * share)], drecv_sem.at[3])

        @pl.when(head != 0)
        def _():
            arrived(tiles, drecv_sem.at[3])

        wide = [tiles[p].astype(jnp.float32) for p in range(seq_size)]
        for d in range(reach):
            picked = jnp.zeros(wide[0].shape, jnp.float32)
            for p in range(seq_size):
                picked = picked + jnp.where(place_ref[p] == seq + d - margin, 1.0, 0.0) * wide[p]
            for f in range(frames):
                chosen = picked[:, f, :].astype(jnp.bfloat16)
                for c in range(pieces + 1):
                    active = silu(lifted(chosen, lifts[c], biases[c])) * inside(d - margin)
                    act1[f, d, :, c * own:(c + 1) * own] = active.astype(jnp.bfloat16)
                if 1 <= d <= reach - 2:
                    feat[f, d - 1] = lifted(chosen, lifts[quarter], biases[quarter])

        tap_copy.wait()
        convolve(0, act1, reach - 2)
        for f in range(frames):
            for r in range(reach - 2):
                value = feat[f, r] + gathered_columns(f, r)
                feat[f, r] = value
                act2[f, r, :, own_lanes] = (silu(value) * inside(r + 1 - margin)).astype(jnp.bfloat16)
        for mate in mates:
            send(act2.at[:, :, :, own_lanes], act2.at[:, :, :, own_lanes], 4, mate)

    def last_layer():
        arrived(act2.at[:, :, :, pl.ds(0, pieces * own)], drecv_sem.at[4])
        convolve(1, act2, reach - 4)
        for f in range(frames):
            dec_ref[pl.ds(f, own, stride=frames), :] = jnp.transpose(
                feat[f, margin - 1] + gathered_columns(f, 0)
            )

    def give(h, target, r):
        start = pl.multiple_of(target * block + r * rows, rows)
        pltpu.make_async_remote_copy(
            src_ref=obuf.at[h, pl.ds(start, rows), :],
            dst_ref=att.at[:, block_of(h, me)],
            send_sem=osend_sem,
            recv_sem=orecv_sem.at[h * count + me],
            device_id={"seq": target, "rep": r},
            device_id_type=MESH,
        ).start()

    block = rep_size * rows
    for h in range(own_heads):
        arrived(qkv.at[h, :, pl.ds(0, others * rows), :], recv_sem.at[h])

        def attend(step, carry):
            target = jnp.where(
                step % 2 == 0, far + step // 2, jnp.where(step == 1, mirror, seq)
            )
            here = pl.ds(pl.multiple_of(target * block, block), block)
            scores = lax.dot_general(
                qkv[h, 0, here, :], qkv[h, 1], (((1,), (1,)), ((), ())),
                preferred_element_type=jnp.float32,
            ) * factor
            exponent = jnp.exp(scores - jnp.max(scores, axis=1, keepdims=True))
            total = jnp.sum(exponent, axis=1, keepdims=True)
            summed = jnp.dot(
                exponent.astype(jnp.bfloat16), qkv[h, 2], preferred_element_type=jnp.float32
            )
            obuf[h, here, :] = (summed / total).astype(jnp.bfloat16)
            inner_far = jnp.logical_and(step % 2 == 0, seq == inner)
            for r in range(rep_size):
                other = jnp.logical_or(target != seq, rep != r)
                if h < own_heads - 1:
                    other = jnp.logical_and(other, jnp.logical_not(inner_far))
                else:
                    @pl.when(inner_far)
                    def _():
                        for e in range(own_heads - 1):
                            give(e, target, r)

                @pl.when(other)
                def _():
                    give(h, target, r)
            return carry

        lax.fori_loop(0, seq_size, attend, 0)
        att[:, block_of(h, me)] = obuf[h, my_rows, :]
        if h == 0:
            first_layer()
        if h == 1:
            last_layer()

    for side in sides[4:]:
        side.wait()
    latent = lat_ref.shape[0]
    squares = jnp.zeros((rows, HEAD_DIM), jnp.float32)
    projected = jnp.zeros((latent, rows), jnp.float32)
    for h, step in [
        (h, half * across + step)
        for across in (1, 0) for h in range(own_heads) for step in range(half)
    ]:
        for r in range(rep_size):
            origin = lax.rem(far + step, seq_size) * rep_size + r

            @pl.when(origin != me)
            def _():
                arrived(obuf.at[h, pl.ds(0, rows), :], orecv_sem.at[h * count + origin])

            cols = block_of(h, origin)
            combined = (
                stream_ref[:, cols].astype(jnp.float32) + att[:, cols].astype(jnp.float32)
            )
            hidden = combined.astype(jnp.bfloat16)
            hid_ref[:, cols] = hidden
            widened = hidden.astype(jnp.float32)
            squares = squares + widened * widened
            scaled = (widened * gain_ref[:, cols]).astype(jnp.bfloat16)
            projected = projected + lax.dot_general(
                lw_ref[:, cols], scaled, (((1,), (1,)), ((), ())),
                preferred_element_type=jnp.float32,
            )
    summed = jnp.sum(jnp.transpose(squares), axis=0, keepdims=True)
    part[:latent] = projected.astype(jnp.bfloat16)
    part[latent:] = jnp.broadcast_to(summed, (part.shape[0] - latent, rows)).astype(jnp.bfloat16)
    swap = pltpu.make_async_remote_copy(
        src_ref=part, dst_ref=part_in, send_sem=psend_sem, recv_sem=precv_sem,
        device_id={"head": lax.rem(head + 1, head_size)}, device_id_type=MESH,
    )
    swap.start()
    arrived(qkv.at[:, :, pl.ds(0, others * rows), :], send_sem)
    arrived(obuf.at[:, pl.ds(0, others * rows), :], osend_sem)
    arrived(lifts.at[pl.ds(0, pieces)], dsend_sem.at[1])
    arrived(biases.at[pl.ds(0, pieces)], dsend_sem.at[2])

    @pl.when(head == 0)
    def _():
        arrived(tiles.at[pl.ds(0, 2), pl.ds(0, share)], dsend_sem.at[0])
        told = pieces * seq_size * share * frames * columns_here // HEAD_DIM
        arrived(obuf.at[0, pl.ds(0, told), :], dsend_sem.at[3])

        @pl.when(seq == inner)
        def _():
            arrived(far_tiles, dsend_sem.at[5])

    arrived(act2.at[:, :, :, pl.ds(0, pieces * own)], dsend_sem.at[4])
    swap.wait()
    both = part[...].astype(jnp.float32) + part_in[...].astype(jnp.float32)
    lat_ref[...] = both[:latent] * lax.rsqrt(both[latent:latent + 1] / full_width + epsilon)


def finish_kernel(hid_in, lat_in, dec_in, hid_out, lat_out, dec_out, sem):
    writes = [
        pltpu.make_async_copy(held, out, sem.at[i])
        for i, (held, out) in enumerate(
            ((hid_in, hid_out), (lat_in, lat_out), (dec_in, dec_out))
        )
    ]
    for write in writes:
        write.start()
    for write in writes:
        write.wait()


def fused(
    queries, key_tokens, value_tokens, stream, norm_gain, latent_weight,
    tile_pool, tile_position, lift_weight, lift_bias, conv_weight,
):
    seq_size, rep_size, head_size = (lax.axis_size(a) for a in ("seq", "rep", "head"))
    rows, width = queries.shape
    count = seq_size * rep_size
    own_heads = width // HEAD_DIM // count
    latent = latent_weight.shape[1]
    depth, frames, columns = tile_pool.shape[1:]
    layers, _, own, channels = conv_weight.shape
    quarters = head_size * rep_size
    reach = 2 * layers + 1
    bf = jnp.bfloat16
    vmem = pl.BlockSpec(memory_space=pltpu.VMEM)
    hbm = pl.BlockSpec(memory_space=pltpu.HBM)
    dma = pltpu.SemaphoreType.DMA
    held = (
        pltpu.VMEM((rows, width), bf),
        pltpu.VMEM((latent, rows), jnp.float32),
        pltpu.VMEM((own * frames, columns), jnp.float32),
    )
    hidden, latents, decoded = pl.pallas_call(
        functools.partial(fused_kernel, seq_size, rep_size, head_size, width * head_size),
        out_shape=held,
        in_specs=[hbm] * 11,
        out_specs=(vmem, vmem, vmem),
        scratch_shapes=[pltpu.VMEM((rows, width), bf)] * 4 + [
            pltpu.VMEM((1, width), jnp.float32),
            pltpu.VMEM((latent, width), bf),
            pltpu.SMEM(tile_position.shape, jnp.int32),
            pltpu.VMEM((own_heads, 3, count * rows, HEAD_DIM), bf),
            pltpu.VMEM((own_heads, count * rows, HEAD_DIM), bf),
            pltpu.VMEM((rows, width), bf),
            pltpu.VMEM((latent + 16, rows), bf),
            pltpu.VMEM((latent + 16, rows), bf),
            pltpu.VMEM((seq_size, depth, frames, columns), bf),
            pltpu.VMEM((quarters, depth, own), bf),
            pltpu.VMEM((quarters, 1, own), jnp.float32),
            pltpu.VMEM(conv_weight.shape, bf),
            pltpu.VMEM((frames, reach, columns, channels), bf),
            pltpu.VMEM((frames, reach - 2, columns, channels), bf),
            pltpu.VMEM((frames, reach - 2, columns, own), jnp.float32),
            pltpu.VMEM((frames, (reach - 2) * columns, 3 * own), jnp.float32),
            pltpu.SemaphoreType.REGULAR((seq_size - 1,)),
            pltpu.SemaphoreType.REGULAR((head_size - 1,)),
            dma, dma((own_heads,)), dma, dma((own_heads * count,)), dma, dma,
            dma((3 * own_heads,)), dma((7,)), dma, dma((6,)), dma((5,)),
        ],
        compiler_params=pltpu.CompilerParams(
            collective_id=0, has_side_effects=True, vmem_limit_bytes=48 << 20
        ),
    )(*(
        pltpu.with_memory_space_constraint(operand, pltpu.HBM) for operand in (
            queries, key_tokens, value_tokens, stream, norm_gain[None, :], latent_weight.T,
            tile_pool, tile_position, lift_weight, lift_bias[None, :], conv_weight,
        )
    ))
    hidden, latents, decoded = pl.pallas_call(
        finish_kernel,
        out_shape=tuple(jax.ShapeDtypeStruct(ref.shape, ref.dtype) for ref in held),
        in_specs=[vmem, vmem, vmem],
        out_specs=(hbm, hbm, hbm),
        scratch_shapes=[dma((3,))],
        compiler_params=pltpu.CompilerParams(vmem_limit_bytes=8 << 20),
    )(hidden, latents, decoded)
    return hidden, latents.T, decoded.reshape(own, frames, 1, columns)


def gathered(queries, key_tokens, value_tokens, stream, norm_gain, latent_weight):
    query_heads, initial = prepare(queries)
    state = make_update(
        query_heads,
        initial,
        (
            lax.all_gather(key_tokens, ("seq", "rep"), axis=0, tiled=True),
            lax.all_gather(value_tokens, ("seq", "rep"), axis=0, tiled=True),
        ),
    )
    attended = finish(state)
    combined = stream.astype(jnp.float32) + attended.astype(jnp.float32)
    hidden = combined.astype(jnp.bfloat16)
    widened = hidden.astype(jnp.float32)
    scaled = (widened * norm_gain).astype(jnp.bfloat16)
    partial_proj = jnp.dot(scaled, latent_weight, preferred_element_type=jnp.float32)
    partial_squares = jnp.sum(widened * widened, axis=1)
    projected, squares = (
        lax.psum(partial_proj.astype(jnp.bfloat16), "head").astype(jnp.float32),
        lax.psum(partial_squares.astype(jnp.bfloat16), "head").astype(jnp.float32),
    )
    latents = projected * lax.rsqrt(squares / WIDTH + epsilon)[:, None]
    return hidden, latents


def shards(
    queries,
    key_tokens,
    value_tokens,
    stream,
    norm_gain,
    latent_weight,
    tile_pool,
    tile_position,
    lift_weight,
    lift_bias,
    conv_weight,
):
    heads_here = queries.shape[1] // HEAD_DIM
    spread = lax.axis_size("seq") * lax.axis_size("rep")
    fits = heads_here % spread == 0 and lax.axis_size("seq") == 4 and lax.axis_size("head") == 2
    fits = fits and lax.axis_size("rep") == 2 and tile_pool.shape[0] == 1
    fits = fits and conv_weight.shape[0] == 2 and lift_weight.shape[0] % 64 == 0
    if fits:
        return fused(
            queries, key_tokens, value_tokens, stream, norm_gain, latent_weight,
            tile_pool, tile_position, lift_weight, lift_bias, conv_weight,
        )
    hidden, latents = gathered(
        queries, key_tokens, value_tokens, stream, norm_gain, latent_weight
    )
    tiles_here = tile_pool.shape[0]
    frames = tile_pool.shape[2]
    columns = tile_pool.shape[3]
    own_rows = lax.axis_index("seq") * tiles_here + jnp.arange(tiles_here, dtype=jnp.int32)
    collected = make_pick(
        tile_position, own_rows, lax.all_gather(tile_pool, "seq", axis=0, tiled=True)
    )
    latent_grid = collected.astype(jnp.bfloat16)
    channels_here = lift_weight.shape[1]
    feature_map = (
        lax.dot_general(
            lift_weight,
            latent_grid.reshape(latent_grid.shape[0], -1),
            (((0,), (0,)), ((), ())),
            preferred_element_type=jnp.float32,
        )
        + lift_bias[:, None]
    )
    for layer_index in range(conv_weight.shape[0]):
        layer_weight = conv_weight[layer_index]
        active = (
            jax.nn.silu(feature_map)
            .astype(jnp.bfloat16)
            .reshape(channels_here, frames, tiles_here, columns)
        )
        zeros_here = jnp.zeros(feature_map.shape, jnp.float32)
        bordered = padded(active, (("seq", 2),), 1)
        rimmed = lax.all_gather(bordered, ("head", "rep"), axis=0, tiled=True)
        update = tap_sum(zeros_here, rimmed, layer_weight)
        feature_map = feature_map + update
    decoded = feature_map.reshape(channels_here, frames, tiles_here, columns)
    return (hidden, latents, decoded)


def solution(mesh):
    in_specs = (
        P(("groups", "seq", "rep"), "head"),
        P(("groups", "seq", "rep"), "head"),
        P(("groups", "seq", "rep"), "head"),
        P(("groups", "seq", "rep"), "head"),
        P("head"),
        P("head", None),
        P(("groups", "seq"), None, None, None),
        P("groups"),
        P(None, ("head", "rep")),
        P(("head", "rep")),
        P(None, None, ("head", "rep"), None),
    )
    out_specs = (
        P(("groups", "seq", "rep"), "head"),
        P(("groups", "seq", "rep"), None),
        P(("groups", "head", "rep"), None, "seq", None),
    )
    return jax.shard_map(shards, mesh=mesh, in_specs=in_specs, out_specs=out_specs, check_vma=False)
```

```python
import functools
import math

import jax
import jax.numpy as jnp
from jax import lax
from jax.experimental import pallas as pl
from jax.experimental.pallas import tpu as pltpu
from jax.sharding import PartitionSpec as P

HEAD_DIM = 128
WIDTH = 6144


epsilon = 1e-06
negative = -1e30


def padded(shard, sides, width):
    for axis, dim in sides:
        peers, length = (lax.axis_size(axis), shard.shape[dim])
        up = [(i, (i + 1) % peers) for i in range(peers - 1)]
        down = [(j, i) for i, j in up]
        last = lax.slice_in_dim(shard, length - width, length, axis=dim)
        leading = lax.slice_in_dim(shard, 0, width, axis=dim)
        before = lax.ppermute(last, axis, up)
        after = lax.ppermute(leading, axis, down)
        shard = jnp.concatenate([before, shard, after], axis=dim)
    return shard


def prepare(block_rows):
    row_count = block_rows.shape[0]
    head_count = block_rows.shape[1] // HEAD_DIM
    query_heads = block_rows.reshape(row_count, head_count, HEAD_DIM)
    initial = (
        jnp.full((head_count, row_count), negative, jnp.float32),
        jnp.zeros((head_count, row_count), jnp.float32),
        jnp.zeros((head_count, row_count, HEAD_DIM), jnp.float32),
    )
    return (query_heads, initial)


def make_update(query_heads, state, pieces):
    head_count = query_heads.shape[1]
    factor = 1.0 / math.sqrt(HEAD_DIM)
    running_max, running_sum, accum = state
    key_piece, value_piece = pieces
    piece_rows = key_piece.shape[0]
    key_heads = key_piece.reshape(piece_rows, head_count, HEAD_DIM)
    value_heads = value_piece.reshape(piece_rows, head_count, HEAD_DIM)
    scores = (
        jnp.einsum("qhd,khd->hqk", query_heads, key_heads, preferred_element_type=jnp.float32)
        * factor
    )
    new_max = jnp.maximum(running_max, jnp.max(scores, axis=2))
    exponent = jnp.exp(scores - new_max[:, :, None])
    running_sum = jnp.sum(exponent, axis=2)
    accum = jnp.einsum(
        "hqk,khd->hqd",
        exponent.astype(jnp.bfloat16),
        value_heads,
        preferred_element_type=jnp.float32,
    )
    return (new_max, running_sum, accum)


def finish(state):
    running_max, running_sum, accum = state
    result = accum / running_sum[:, :, None]
    return jnp.transpose(result, (1, 0, 2)).reshape(result.shape[1], -1).astype(jnp.bfloat16)


def shift_columns(window, col_shift):
    if col_shift == 0:
        return window
    edge = jnp.zeros(window.shape[:-1] + (1,), window.dtype)
    if col_shift < 0:
        return jnp.concatenate([edge, window[..., :-1]], axis=-1)
    return jnp.concatenate([window[..., 1:], edge], axis=-1)


def tap_sum(running, piece_block, layer_weight):
    piece_rows = piece_block.shape[0]
    frames = piece_block.shape[1]
    band_rows = piece_block.shape[2] - 2
    framed = jnp.pad(piece_block, ((0, 0), (1, 1), (0, 0), (0, 0)))
    for frame_off in range(3):
        for row_off in range(3):
            for col_off in range(3):
                window = shift_columns(
                    framed[:, frame_off : frame_off + frames, row_off : row_off + band_rows, :],
                    col_off - 1,
                )
                tap_weight = layer_weight[frame_off * 9 + row_off * 3 + col_off]
                running = running + lax.dot_general(
                    tap_weight,
                    window.reshape(piece_rows, -1),
                    (((1,), (0,)), ((), ())),
                    preferred_element_type=jnp.float32,
                )
    return running


def make_pick(tile_position, own_rows, piece_block):
    selector = (own_rows[:, None] == tile_position[None, :]).astype(jnp.bfloat16)
    return jnp.einsum("tp,plfc->lftc", selector, piece_block, preferred_element_type=jnp.float32)


MESH = pl.DeviceIdType.MESH


def fused_kernel(
    seq_size, rep_size, head_size, full_width,
    q_hbm, k_hbm, v_hbm, stream_hbm, gain_hbm, lw_hbm,
    tile_hbm, place_hbm, lift_hbm, bias_hbm, conv_hbm,
    hid_ref, lat_ref, dec_ref,
    q_ref, k_ref, v_ref, stream_ref, gain_ref, lw_ref, place_ref,
    qkv, obuf, att, part, part_in,
    tiles, lifts, biases, taps, act1, act2, feat, acc,
    ready, ready_mate,
    send_sem, recv_sem, osend_sem, orecv_sem, psend_sem, precv_sem,
    load_sem, side_sem, tap_sem, dsend_sem, drecv_sem,
):
    seq, rep, head = (lax.axis_index(a) for a in ("seq", "rep", "head"))
    count = seq_size * rep_size
    me = seq * rep_size + rep
    rows = q_ref.shape[0]
    own_heads = qkv.shape[0]
    others = count - 1
    factor = 1.0 / math.sqrt(HEAD_DIM)
    quarter = head * rep_size + rep
    sources = (q_ref, k_ref, v_ref)

    stretch = count * HEAD_DIM
    loads = []
    for h in range(own_heads):
        cols = pl.ds(h * stretch, stretch)
        loads.append([
            pltpu.make_async_copy(origin.at[:, cols], source.at[:, cols], load_sem.at[i if h == 0 else 3])
            for i, (origin, source) in enumerate(zip((q_hbm, k_hbm, v_hbm), sources))
        ])
    for load in loads[0]:
        load.start()

    barrier = pltpu.get_barrier_semaphore()
    for e in range(1, rep_size):
        pl.semaphore_signal(
            barrier, inc=1, device_id={"rep": lax.rem(rep + e, rep_size)}, device_id_type=MESH
        )
    for k in range(1, seq_size):
        @pl.when(seq + k < seq_size)
        def _():
            for r in range(rep_size):
                pl.semaphore_signal(
                    barrier, inc=1, device_id={"seq": seq + k, "rep": r}, device_id_type=MESH
                )
    half = seq_size // 2

    @pl.when(seq == half)
    def _():
        for r in range(rep_size):
            pl.semaphore_signal(
                barrier, inc=1, device_id={"seq": seq - 1, "rep": r}, device_id_type=MESH
            )

    for k in range(1, head_size):
        @pl.when(head + k < head_size)
        def _():
            for r in range(rep_size):
                pl.semaphore_signal(
                    barrier, inc=1, device_id={"head": head + k, "rep": r}, device_id_type=MESH
                )
    greeted = seq + head + jnp.where(seq == half - 1, 1, 0)
    pl.semaphore_wait(barrier, rep_size - 1 + rep_size * greeted)
    for k in range(1, seq_size):
        @pl.when(jnp.logical_and(seq >= k, jnp.logical_or(k > 1, seq != half)))
        def _():
            for r in range(rep_size):
                pl.semaphore_signal(
                    ready.at[k - 1], inc=1, device_id={"seq": seq - k, "rep": r},
                    device_id_type=MESH,
                )
    for k in range(1, head_size):
        @pl.when(head >= k)
        def _():
            for r in range(rep_size):
                pl.semaphore_signal(
                    ready_mate.at[k - 1], inc=1, device_id={"head": head - k, "rep": r},
                    device_id_type=MESH,
                )

    upper = seq // half
    far = (1 - upper) * half
    inner = upper * half + (1 - upper) * (half - 1)
    mirror = 2 * half * upper + half - 1 - seq
    share = tiles.shape[1] // rep_size
    my_share = pl.ds(pl.multiple_of(rep * share, share), share)
    sides = [
        pltpu.make_async_copy(origin, target, side_sem.at[i])
        for i, (origin, target) in enumerate((
            (tile_hbm.at[0, my_share], tiles.at[seq, my_share]),
            (lift_hbm, lifts.at[quarter]),
            (bias_hbm, biases.at[quarter]),
            (place_hbm, place_ref),
            (stream_hbm, stream_ref),
            (gain_hbm, gain_ref),
            (lw_hbm, lw_ref),
        ))
    ]
    @pl.when(head == 0)
    def _():
        sides[0].start()


    def arrived(ref, sem):
        pltpu.make_async_copy(ref, ref, sem).wait()

    def send(source, target, index, device):
        pltpu.make_async_remote_copy(
            src_ref=source, dst_ref=target,
            send_sem=dsend_sem.at[index], recv_sem=drecv_sem.at[index],
            device_id=device, device_id_type=MESH,
        ).start()

    my_rows = pl.ds(pl.multiple_of(me * rows, rows), rows)

    def block_of(h, place):
        return pl.ds(pl.multiple_of((h * count + place) * HEAD_DIM, HEAD_DIM), HEAD_DIM)

    def send_one(h, i, target, r):
        pltpu.make_async_remote_copy(
            src_ref=sources[i].at[:, block_of(h, target * rep_size + r)],
            dst_ref=qkv.at[h, i, my_rows, :],
            send_sem=send_sem,
            recv_sem=recv_sem.at[h],
            device_id={"seq": target, "rep": r},
            device_id_type=MESH,
        ).start()

    def send_back(h, arrays):
        for k in (2, 1, 3):
            @pl.when(seq >= k)
            def _():
                for r in range(rep_size):
                    for i in arrays:
                        send_one(h, i, seq - k, r)

    def send_on(h):
        for k in range(1, seq_size):
            @pl.when(seq + k < seq_size)
            def _():
                if h == 0:
                    @pl.when(jnp.logical_or(k > 1, seq != half - 1))
                    def _():
                        pl.semaphore_wait(ready.at[k - 1], rep_size)

                for r in range(rep_size):
                    for i in range(3):
                        send_one(h, i, seq + k, r)
        for e in range(1, rep_size):
            for i in range(3):
                send_one(h, i, seq, lax.rem(rep + e, rep_size))

    own_tile = tiles.at[seq, my_share]
    far_tiles = tiles.at[pl.ds(far, half), my_share]
    for i, load in enumerate(loads[0]):
        load.wait()
        send_back(0, (i,))
    for pending in loads[1:]:
        for load in pending:
            load.start()
    send_on(0)

    @pl.when(head == 0)
    def _():
        sides[0].wait()
        send(own_tile, own_tile, 0, {"seq": mirror})
        send(own_tile, own_tile, 0, {"seq": (1 - upper) * half + upper * (half - 1)})

    tap_copy = pltpu.make_async_copy(conv_hbm, taps, tap_sem)
    tap_copy.start()
    for side in sides[1:]:
        side.start()
    arrived(qkv.at[pl.ds(1, own_heads - 1), :, pl.ds(0, count * rows), :], load_sem.at[3])
    for h in range(1, own_heads):
        send_back(h, range(3))
        send_on(h)

    @pl.when(head == 0)
    def _():
        @pl.when(seq == inner)
        def _():
            arrived(tiles.at[pl.ds(0, seq_size - 1), pl.ds(0, share)], drecv_sem.at[0])
            pltpu.make_async_remote_copy(
                src_ref=far_tiles, dst_ref=far_tiles,
                send_sem=dsend_sem.at[5], recv_sem=drecv_sem.at[0],
                device_id={"seq": mirror}, device_id_type=MESH,
            ).start()

    mates = [
        {"head": lax.rem(head + d, head_size), "rep": lax.rem(rep + e, rep_size)}
        for d in range(head_size) for e in range(rep_size) if (d, e) != (0, 0)
    ]
    for k in range(1, head_size):
        @pl.when(head + k < head_size)
        def _():
            pl.semaphore_wait(ready_mate.at[k - 1], rep_size)
    sides[1].wait()
    sides[2].wait()
    for mate in mates:
        send(lifts.at[quarter], lifts.at[quarter], 1, mate)
        send(biases.at[quarter], biases.at[quarter], 2, mate)
    pieces = len(mates)
    for h in range(own_heads):
        columns = block_of(h, me)
        for i, source in enumerate(sources):
            qkv[h, i, my_rows, :] = source[:, columns]
    frames, reach, columns_here, channels = act1.shape
    own = lifts.shape[2]
    margin = reach // 2
    own_lanes = pl.ds(pl.multiple_of(quarter * own, own), own)

    def inside(d):
        row = seq + d
        return jnp.where(jnp.logical_and(row >= 0, row < seq_size), 1.0, 0.0)

    def silu(value):
        return value / (1.0 + jnp.exp(-value))

    def lifted(chosen, weight, bias):
        return lax.dot_general(
            chosen, weight, (((0,), (0,)), ((), ())), preferred_element_type=jnp.float32
        ) + bias

    def convolve(layer, active, rows_out):
        length = rows_out * columns_here
        for f in range(frames):
            first = True
            for a in range(3):
                if not 0 <= f + a - 1 < frames:
                    continue
                for b in range(3):
                    window = active[f + a - 1, b:b + rows_out].reshape(length, channels)
                    base = 9 * a + 3 * b
                    term = lax.dot_general(
                        window, taps[layer, base:base + 3].reshape(3 * own, channels),
                        (((1,), (1,)), ((), ())), preferred_element_type=jnp.float32,
                    )
                    acc[f, :length, :] = term if first else acc[f, :length, :] + term
                    first = False

    def gathered_columns(f, r):
        lines = slice(r * columns_here, (r + 1) * columns_here)
        at = lax.broadcasted_iota(jnp.int32, (columns_here, own), 0)
        before = pltpu.roll(acc[f, lines, :own], 1, 0)
        after = pltpu.roll(acc[f, lines, 2 * own:], columns_here - 1, 0)
        return (
            acc[f, lines, own:2 * own]
            + jnp.where(at == 0, 0.0, before)
            + jnp.where(at == columns_here - 1, 0.0, after)
        )

    def first_layer():
        @pl.when(head == 0)
        def _():
            @pl.when(seq != inner)
            def _():
                arrived(tiles.at[pl.ds(0, seq_size - 1), pl.ds(0, share)], drecv_sem.at[0])

            for mate in mates:
                send(tiles.at[:, my_share], tiles.at[:, my_share], 3, mate)

        sides[3].wait()
        arrived(lifts.at[pl.ds(0, pieces)], drecv_sem.at[1])
        arrived(biases.at[pl.ds(0, pieces)], drecv_sem.at[2])
        @pl.when(head == 0)
        def _():
            arrived(tiles.at[:, pl.ds(0, (rep_size - 1) * share)], drecv_sem.at[3])

        @pl.when(head != 0)
        def _():
            arrived(tiles, drecv_sem.at[3])

        wide = [tiles[p].astype(jnp.float32) for p in range(seq_size)]
        for d in range(reach):
            picked = jnp.zeros(wide[0].shape, jnp.float32)
            for p in range(seq_size):
                picked = picked + jnp.where(place_ref[p] == seq + d - margin, 1.0, 0.0) * wide[p]
            for f in range(frames):
                chosen = picked[:, f, :].astype(jnp.bfloat16)
                for c in range(pieces + 1):
                    active = silu(lifted(chosen, lifts[c], biases[c])) * inside(d - margin)
                    act1[f, d, :, c * own:(c + 1) * own] = active.astype(jnp.bfloat16)
                if 1 <= d <= reach - 2:
                    feat[f, d - 1] = lifted(chosen, lifts[quarter], biases[quarter])

        tap_copy.wait()
        convolve(0, act1, reach - 2)
        for f in range(frames):
            for r in range(reach - 2):
                value = feat[f, r] + gathered_columns(f, r)
                feat[f, r] = value
                act2[f, r, :, own_lanes] = (silu(value) * inside(r + 1 - margin)).astype(jnp.bfloat16)
        for mate in mates:
            send(act2.at[:, :, :, own_lanes], act2.at[:, :, :, own_lanes], 4, mate)

    def last_layer():
        arrived(act2.at[:, :, :, pl.ds(0, pieces * own)], drecv_sem.at[4])
        convolve(1, act2, reach - 4)
        for f in range(frames):
            dec_ref[pl.ds(f, own, stride=frames), :] = jnp.transpose(
                feat[f, margin - 1] + gathered_columns(f, 0)
            )

    def give(h, target, r):
        group = jnp.where(target // half == upper, 0, jnp.where(seq == inner, 2 + h, 1))
        start = pl.multiple_of(target * block + r * rows, rows)
        pltpu.make_async_remote_copy(
            src_ref=obuf.at[h, pl.ds(start, rows), :],
            dst_ref=att.at[:, block_of(h, me)],
            send_sem=osend_sem,
            recv_sem=orecv_sem.at[group],
            device_id={"seq": target, "rep": r},
            device_id_type=MESH,
        ).start()

    block = rep_size * rows
    for h in range(own_heads):
        arrived(qkv.at[h, :, pl.ds(0, others * rows), :], recv_sem.at[h])

        def attend(step, carry):
            target = jnp.where(
                step % 2 == 0, far + step // 2, jnp.where(step == 1, mirror, seq)
            )
            here = pl.ds(pl.multiple_of(target * block, block), block)
            scores = lax.dot_general(
                qkv[h, 0, here, :], qkv[h, 1], (((1,), (1,)), ((), ())),
                preferred_element_type=jnp.float32,
            ) * factor
            exponent = jnp.exp(scores - jnp.max(scores, axis=1, keepdims=True))
            total = jnp.sum(exponent, axis=1, keepdims=True)
            summed = jnp.dot(
                exponent.astype(jnp.bfloat16), qkv[h, 2], preferred_element_type=jnp.float32
            )
            obuf[h, here, :] = (summed / total).astype(jnp.bfloat16)
            inner_far = jnp.logical_and(step % 2 == 0, seq == inner)
            for r in range(rep_size):
                other = jnp.logical_or(target != seq, rep != r)
                if h < own_heads - 1:
                    other = jnp.logical_and(other, jnp.logical_not(inner_far))
                else:
                    @pl.when(inner_far)
                    def _():
                        for e in range(own_heads - 1):
                            give(e, target, r)

                @pl.when(other)
                def _():
                    give(h, target, r)
            return carry

        lax.fori_loop(0, seq_size, attend, 0)
        att[:, block_of(h, me)] = obuf[h, my_rows, :]
        if h == 0:
            first_layer()
        if h == 1:
            last_layer()

    for side in sides[4:]:
        side.wait()
    latent = lat_ref.shape[0]
    squares = jnp.zeros((rows, HEAD_DIM), jnp.float32)
    projected = jnp.zeros((latent, rows), jnp.float32)
    plan = (
        [(h, chip, 0) for h in range(own_heads) for chip in (seq, mirror)]
        + [(h, far + 1 - upper, 1) for h in range(own_heads)]
        + [(h, far + upper, 2 + h) for h in range(own_heads)]
    )
    waited = set()
    for h, chip, group in plan:
        if group not in waited:
            waited.add(group)
            if group == 0:
                came = obuf.at[:, pl.ds(0, (half * rep_size - 1) * rows), :]
            elif group == 1:
                came = obuf.at[:, pl.ds(0, rep_size * rows), :]
            else:
                came = obuf.at[h, pl.ds(0, rep_size * rows), :]
            arrived(came, orecv_sem.at[group])
        for r in range(rep_size):
            origin = chip * rep_size + r
            cols = block_of(h, origin)
            combined = (
                stream_ref[:, cols].astype(jnp.float32) + att[:, cols].astype(jnp.float32)
            )
            hidden = combined.astype(jnp.bfloat16)
            hid_ref[:, cols] = hidden
            widened = hidden.astype(jnp.float32)
            squares = squares + widened * widened
            scaled = (widened * gain_ref[:, cols]).astype(jnp.bfloat16)
            projected = projected + lax.dot_general(
                lw_ref[:, cols], scaled, (((1,), (1,)), ((), ())),
                preferred_element_type=jnp.float32,
            )
    summed = jnp.sum(jnp.transpose(squares), axis=0, keepdims=True)
    part[:latent] = projected.astype(jnp.bfloat16)
    part[latent:] = jnp.broadcast_to(summed, (part.shape[0] - latent, rows)).astype(jnp.bfloat16)
    swap = pltpu.make_async_remote_copy(
        src_ref=part, dst_ref=part_in, send_sem=psend_sem, recv_sem=precv_sem,
        device_id={"head": lax.rem(head + 1, head_size)}, device_id_type=MESH,
    )
    swap.start()
    arrived(qkv.at[:, :, pl.ds(0, others * rows), :], send_sem)
    arrived(obuf.at[:, pl.ds(0, others * rows), :], osend_sem)
    arrived(lifts.at[pl.ds(0, pieces)], dsend_sem.at[1])
    arrived(biases.at[pl.ds(0, pieces)], dsend_sem.at[2])

    @pl.when(head == 0)
    def _():
        arrived(tiles.at[pl.ds(0, 2), pl.ds(0, share)], dsend_sem.at[0])
        told = pieces * seq_size * share * frames * columns_here // HEAD_DIM
        arrived(obuf.at[0, pl.ds(0, told), :], dsend_sem.at[3])

        @pl.when(seq == inner)
        def _():
            arrived(far_tiles, dsend_sem.at[5])

    arrived(act2.at[:, :, :, pl.ds(0, pieces * own)], dsend_sem.at[4])
    swap.wait()
    both = part[...].astype(jnp.float32) + part_in[...].astype(jnp.float32)
    lat_ref[...] = both[:latent] * lax.rsqrt(both[latent:latent + 1] / full_width + epsilon)


def finish_kernel(hid_in, lat_in, dec_in, hid_out, lat_out, dec_out, sem):
    writes = [
        pltpu.make_async_copy(held, out, sem.at[i])
        for i, (held, out) in enumerate(
            ((hid_in, hid_out), (lat_in, lat_out), (dec_in, dec_out))
        )
    ]
    for write in writes:
        write.start()
    for write in writes:
        write.wait()


def fused(
    queries, key_tokens, value_tokens, stream, norm_gain, latent_weight,
    tile_pool, tile_position, lift_weight, lift_bias, conv_weight,
):
    seq_size, rep_size, head_size = (lax.axis_size(a) for a in ("seq", "rep", "head"))
    rows, width = queries.shape
    count = seq_size * rep_size
    own_heads = width // HEAD_DIM // count
    latent = latent_weight.shape[1]
    depth, frames, columns = tile_pool.shape[1:]
    layers, _, own, channels = conv_weight.shape
    quarters = head_size * rep_size
    reach = 2 * layers + 1
    bf = jnp.bfloat16
    vmem = pl.BlockSpec(memory_space=pltpu.VMEM)
    hbm = pl.BlockSpec(memory_space=pltpu.HBM)
    dma = pltpu.SemaphoreType.DMA
    held = (
        pltpu.VMEM((rows, width), bf),
        pltpu.VMEM((latent, rows), jnp.float32),
        pltpu.VMEM((own * frames, columns), jnp.float32),
    )
    hidden, latents, decoded = pl.pallas_call(
        functools.partial(fused_kernel, seq_size, rep_size, head_size, width * head_size),
        out_shape=held,
        in_specs=[hbm] * 11,
        out_specs=(vmem, vmem, vmem),
        scratch_shapes=[pltpu.VMEM((rows, width), bf)] * 4 + [
            pltpu.VMEM((1, width), jnp.float32),
            pltpu.VMEM((latent, width), bf),
            pltpu.SMEM(tile_position.shape, jnp.int32),
            pltpu.VMEM((own_heads, 3, count * rows, HEAD_DIM), bf),
            pltpu.VMEM((own_heads, count * rows, HEAD_DIM), bf),
            pltpu.VMEM((rows, width), bf),
            pltpu.VMEM((latent + 16, rows), bf),
            pltpu.VMEM((latent + 16, rows), bf),
            pltpu.VMEM((seq_size, depth, frames, columns), bf),
            pltpu.VMEM((quarters, depth, own), bf),
            pltpu.VMEM((quarters, 1, own), jnp.float32),
            pltpu.VMEM(conv_weight.shape, bf),
            pltpu.VMEM((frames, reach, columns, channels), bf),
            pltpu.VMEM((frames, reach - 2, columns, channels), bf),
            pltpu.VMEM((frames, reach - 2, columns, own), jnp.float32),
            pltpu.VMEM((frames, (reach - 2) * columns, 3 * own), jnp.float32),
            pltpu.SemaphoreType.REGULAR((seq_size - 1,)),
            pltpu.SemaphoreType.REGULAR((head_size - 1,)),
            dma, dma((own_heads,)), dma, dma((2 + own_heads,)), dma, dma,
            dma((4,)), dma((7,)), dma, dma((6,)), dma((5,)),
        ],
        compiler_params=pltpu.CompilerParams(
            collective_id=0, has_side_effects=True, vmem_limit_bytes=48 << 20
        ),
    )(*(
        pltpu.with_memory_space_constraint(operand, pltpu.HBM) for operand in (
            queries, key_tokens, value_tokens, stream, norm_gain[None, :], latent_weight.T,
            tile_pool, tile_position, lift_weight, lift_bias[None, :], conv_weight,
        )
    ))
    hidden, latents, decoded = pl.pallas_call(
        finish_kernel,
        out_shape=tuple(jax.ShapeDtypeStruct(ref.shape, ref.dtype) for ref in held),
        in_specs=[vmem, vmem, vmem],
        out_specs=(hbm, hbm, hbm),
        scratch_shapes=[dma((3,))],
        compiler_params=pltpu.CompilerParams(vmem_limit_bytes=8 << 20),
    )(hidden, latents, decoded)
    return hidden, latents.T, decoded.reshape(own, frames, 1, columns)


def gathered(queries, key_tokens, value_tokens, stream, norm_gain, latent_weight):
    query_heads, initial = prepare(queries)
    state = make_update(
        query_heads,
        initial,
        (
            lax.all_gather(key_tokens, ("seq", "rep"), axis=0, tiled=True),
            lax.all_gather(value_tokens, ("seq", "rep"), axis=0, tiled=True),
        ),
    )
    attended = finish(state)
    combined = stream.astype(jnp.float32) + attended.astype(jnp.float32)
    hidden = combined.astype(jnp.bfloat16)
    widened = hidden.astype(jnp.float32)
    scaled = (widened * norm_gain).astype(jnp.bfloat16)
    partial_proj = jnp.dot(scaled, latent_weight, preferred_element_type=jnp.float32)
    partial_squares = jnp.sum(widened * widened, axis=1)
    projected, squares = (
        lax.psum(partial_proj.astype(jnp.bfloat16), "head").astype(jnp.float32),
        lax.psum(partial_squares.astype(jnp.bfloat16), "head").astype(jnp.float32),
    )
    latents = projected * lax.rsqrt(squares / WIDTH + epsilon)[:, None]
    return hidden, latents


def shards(
    queries,
    key_tokens,
    value_tokens,
    stream,
    norm_gain,
    latent_weight,
    tile_pool,
    tile_position,
    lift_weight,
    lift_bias,
    conv_weight,
):
    heads_here = queries.shape[1] // HEAD_DIM
    spread = lax.axis_size("seq") * lax.axis_size("rep")
    fits = heads_here % spread == 0 and lax.axis_size("seq") == 4 and lax.axis_size("head") == 2
    fits = fits and lax.axis_size("rep") == 2 and tile_pool.shape[0] == 1
    fits = fits and conv_weight.shape[0] == 2 and lift_weight.shape[0] % 64 == 0
    if fits:
        return fused(
            queries, key_tokens, value_tokens, stream, norm_gain, latent_weight,
            tile_pool, tile_position, lift_weight, lift_bias, conv_weight,
        )
    hidden, latents = gathered(
        queries, key_tokens, value_tokens, stream, norm_gain, latent_weight
    )
    tiles_here = tile_pool.shape[0]
    frames = tile_pool.shape[2]
    columns = tile_pool.shape[3]
    own_rows = lax.axis_index("seq") * tiles_here + jnp.arange(tiles_here, dtype=jnp.int32)
    collected = make_pick(
        tile_position, own_rows, lax.all_gather(tile_pool, "seq", axis=0, tiled=True)
    )
    latent_grid = collected.astype(jnp.bfloat16)
    channels_here = lift_weight.shape[1]
    feature_map = (
        lax.dot_general(
            lift_weight,
            latent_grid.reshape(latent_grid.shape[0], -1),
            (((0,), (0,)), ((), ())),
            preferred_element_type=jnp.float32,
        )
        + lift_bias[:, None]
    )
    for layer_index in range(conv_weight.shape[0]):
        layer_weight = conv_weight[layer_index]
        active = (
            jax.nn.silu(feature_map)
            .astype(jnp.bfloat16)
            .reshape(channels_here, frames, tiles_here, columns)
        )
        zeros_here = jnp.zeros(feature_map.shape, jnp.float32)
        bordered = padded(active, (("seq", 2),), 1)
        rimmed = lax.all_gather(bordered, ("head", "rep"), axis=0, tiled=True)
        update = tap_sum(zeros_here, rimmed, layer_weight)
        feature_map = feature_map + update
    decoded = feature_map.reshape(channels_here, frames, tiles_here, columns)
    return (hidden, latents, decoded)


def solution(mesh):
    in_specs = (
        P(("groups", "seq", "rep"), "head"),
        P(("groups", "seq", "rep"), "head"),
        P(("groups", "seq", "rep"), "head"),
        P(("groups", "seq", "rep"), "head"),
        P("head"),
        P("head", None),
        P(("groups", "seq"), None, None, None),
        P("groups"),
        P(None, ("head", "rep")),
        P(("head", "rep")),
        P(None, None, ("head", "rep"), None),
    )
    out_specs = (
        P(("groups", "seq", "rep"), "head"),
        P(("groups", "seq", "rep"), None),
        P(("groups", "head", "rep"), None, "seq", None),
    )
    return jax.shard_map(shards, mesh=mesh, in_specs=in_specs, out_specs=out_specs, check_vma=False)
```
